32 devices in a mesh: dp: 8 (over y, x, core), tensor: 4 (over z).
Axes of the slice: x: 2, y: 2, z: 4, core: 2. Of those that a mesh axis runs over, the one named last changes fastest.
Arguments:
- hidden_in: bfloat16 [8192, 2048], P(('dp', 'tensor')), may hold values from -6 to 6
- query_proj: bfloat16 [2048, 2048], P('dp', 'tensor'), may hold values from -0.125 to 0.125
- key_proj: bfloat16 [2048, 1024], P('dp', 'tensor'), may hold values from -0.125 to 0.125
- value_proj: bfloat16 [2048, 1024], P('dp', 'tensor'), may hold values from -0.125 to 0.125
- out_proj: bfloat16 [2048, 2048], P('tensor', 'dp'), may hold values from -1 to 1
- gate_proj: bfloat16 [2048, 6144], P('dp', 'tensor'), may hold values from -0.125 to 0.125
- up_proj: bfloat16 [2048, 6144], P('dp', 'tensor'), may hold values from -0.125 to 0.125
- down_proj: bfloat16 [6144, 2048], P('tensor', 'dp'), may hold values from -0.078125 to 0.078125
- attn_norm: float32 [2048], replicated, may hold values from 0.25 to 1.75
- query_norm: float32 [128], replicated, may hold values from 0.25 to 1.75
- key_norm: float32 [128], replicated, may hold values from 0.25 to 1.75
- ffn_norm: float32 [2048], replicated, may hold values from 0.25 to 1.75
- cotangent: bfloat16 [8192, 2048], P(('dp', 'tensor')), may hold values from -6 to 6
Outputs:
- hidden_out: bfloat16 [8192, 2048], P(('dp', 'tensor'))
- dhidden_in: bfloat16 [8192, 2048], P(('dp', 'tensor'))
- dquery_proj: float32 [2048, 2048], P('dp', 'tensor')
- dkey_proj: float32 [2048, 1024], P('dp', 'tensor')
- dvalue_proj: float32 [2048, 1024], P('dp', 'tensor')
- dout_proj: float32 [2048, 2048], P('tensor', 'dp')
- dgate_proj: float32 [2048, 6144], P('dp', 'tensor')
- dup_proj: float32 [2048, 6144], P('dp', 'tensor')
- ddown_proj: float32 [6144, 2048], P('tensor', 'dp')
- dattn_norm: float32 [2048], replicated
- dquery_norm: float32 [128], replicated
- dkey_norm: float32 [128], replicated
- dffn_norm: float32 [2048], replicated
The draws below stay inside these ranges and needn't reach their ends.
All inputs are finite; a program needn't handle non-finite values.
Results may differ from the reference program's by a relative error of at most 0.022.
Values may be sent and summed in bfloat16 or wider, within the bound.
A program may use at most 256 MiB of HBM per device.

```python
import math
import jax
import jax.numpy as jnp
from jax import lax

D = 2048
HEADS = 16
KV_HEADS = 8
HEAD_DIM = 128
FF = 6144
SEQ_LEN = 1024
TOKENS = 8192


def level_of(stream_key, shape, split, smallest, top_value):
    level, own = 1.0, jax.random.fold_in(stream_key, 6)
    for position, blocks in split:
        draws = jnp.exp(jax.random.uniform(jax.random.fold_in(own, position), (blocks,), jnp.float32, smallest / len(split), top_value / len(split)))
        level = level * jnp.repeat(draws, shape[position] // blocks).reshape([-1 if axis == position else 1 for axis in range(len(shape))])
    return level


def centred(own_key, shape, deviation, limit, split=(), kind=jnp.bfloat16):
    values = jax.random.normal(own_key, shape, jnp.float32) * deviation
    if len(split) > 0:
        values = level_of(own_key, shape, split, -0.22, 0.18) * values
    return jnp.clip(values, min=-limit, max=limit).astype(kind)


def setup_inputs(seed: int = 0) -> dict:
    key_of = jax.random.split(jax.random.key(seed), 14)
    return {
        "hidden_in": centred(key_of[0], (TOKENS, D), 1.0, 6.0, ((0, 32),)),
        "query_proj": centred(key_of[1], (D, HEADS * HEAD_DIM), D ** -0.5, 0.125, ((0, 8), (1, 4))),
        "key_proj": centred(key_of[2], (D, KV_HEADS * HEAD_DIM), D ** -0.5, 0.125, ((0, 8), (1, 4))),
        "value_proj": centred(key_of[3], (D, KV_HEADS * HEAD_DIM), D ** -0.5, 0.125, ((0, 8), (1, 4))),
        "out_proj": centred(key_of[4], (HEADS * HEAD_DIM, D), (HEADS * HEAD_DIM // 64) ** -0.5, 1.0, ((0, 4), (1, 8))),
        "gate_proj": centred(key_of[5], (D, FF), D ** -0.5, 0.125, ((0, 8), (1, 4))),
        "up_proj": centred(key_of[6], (D, FF), D ** -0.5, 0.125, ((0, 8), (1, 4))),
        "down_proj": centred(key_of[7], (FF, D), FF ** -0.5, 0.078125, ((0, 4), (1, 8))),
        "attn_norm": jnp.clip(1.0 + 0.15 * jax.random.normal(key_of[8], (D,), jnp.float32), 0.25, 1.75),
        "query_norm": jnp.clip(1.0 + 0.15 * jax.random.normal(key_of[9], (HEAD_DIM,), jnp.float32), 0.25, 1.75),
        "key_norm": jnp.clip(1.0 + 0.15 * jax.random.normal(key_of[10], (HEAD_DIM,), jnp.float32), 0.25, 1.75),
        "ffn_norm": jnp.clip(1.0 + 0.15 * jax.random.normal(key_of[11], (D,), jnp.float32), 0.25, 1.75),
        "cotangent": centred(key_of[12], (TOKENS, D), 1.0, 6.0, ((0, 32),)),
    }


EPSILON = 1e-06
ROPE_BASE = 1000000.0
NEG_FILL = -1e+30

def norm_forward(values, gain):
    inverse = lax.rsqrt(lax.optimization_barrier(jnp.mean(values * values, axis=-1, keepdims=True)) + EPSILON)
    unit_vals = values * inverse
    return (unit_vals * gain, unit_vals, inverse)

def norm_backward(grad_normed, unit_vals, inverse, gain):
    grad_unit = grad_normed * gain
    grad_values = inverse * (grad_unit - unit_vals * lax.optimization_barrier(jnp.mean(grad_unit * unit_vals, axis=-1, keepdims=True)))
    grad_gain = lax.optimization_barrier(jnp.sum((grad_normed * unit_vals).reshape(-1, gain.shape[0]), axis=0))
    return (grad_values, grad_gain)

def rope_tables(positions, width):
    half_width = width // 2
    freqs = ROPE_BASE ** (-(jnp.arange(half_width, dtype=jnp.float32) * (2.0 / width)))
    angles = positions.astype(jnp.float32)[:, None] * freqs[None, :]
    angles = jnp.concatenate([angles, angles], axis=1)
    return (jnp.cos(angles), jnp.sin(angles))

def rotate_half(values):
    half_width = values.shape[-1] // 2
    return jnp.concatenate([-values[..., half_width:], values[..., :half_width]], axis=-1)

def rotate_back(values):
    half_width = values.shape[-1] // 2
    return jnp.concatenate([values[..., half_width:], -values[..., :half_width]], axis=-1)

def reference(hidden_in, query_proj, key_proj, value_proj, out_proj, gate_proj, up_proj, down_proj, attn_norm, query_norm, key_norm, ffn_norm, cotangent):
    groups = HEADS // KV_HEADS
    score_scale = 1.0 / math.sqrt(HEAD_DIM)
    cosine_table, sine_table = rope_tables(jnp.arange(SEQ_LEN), HEAD_DIM)
    cosine_table = cosine_table[:, None, :]
    sine_table = sine_table[:, None, :]
    causal = jnp.arange(SEQ_LEN)[None, :] <= jnp.arange(SEQ_LEN)[:, None]

    def one_sequence(totals, pieces):
        seq_in, seq_cot = pieces
        inputs = seq_in.astype(jnp.float32)
        normed, unit_one, inv_one = norm_forward(inputs, attn_norm)
        normed_bf = normed.astype(jnp.bfloat16)
        queries = jnp.dot(normed_bf, query_proj, preferred_element_type=jnp.float32).reshape(SEQ_LEN, HEADS, HEAD_DIM)
        keys_raw = jnp.dot(normed_bf, key_proj, preferred_element_type=jnp.float32).reshape(SEQ_LEN, KV_HEADS, HEAD_DIM)
        values_bf = jnp.dot(normed_bf, value_proj, preferred_element_type=jnp.float32).astype(jnp.bfloat16).reshape(SEQ_LEN, KV_HEADS, HEAD_DIM)
        query_normed, query_unit, query_inv = norm_forward(queries, query_norm)
        key_normed, key_unit, key_inv = norm_forward(keys_raw, key_norm)
        query_rot = (query_normed * cosine_table + rotate_half(query_normed) * sine_table).astype(jnp.bfloat16)
        query_rot = query_rot.reshape(SEQ_LEN, KV_HEADS, groups, HEAD_DIM)
        key_rot = (key_normed * cosine_table + rotate_half(key_normed) * sine_table).astype(jnp.bfloat16)
        scores = jnp.einsum('qkgd,tkd->kgqt', query_rot.astype(jnp.float32), key_rot.astype(jnp.float32)) * score_scale
        scores = jnp.where(causal, scores, NEG_FILL)
        top_score = lax.optimization_barrier(jnp.max(scores, axis=-1, keepdims=True))
        log_total = top_score + jnp.log(lax.optimization_barrier(jnp.sum(jnp.exp(scores - top_score), axis=-1, keepdims=True)))
        prob_vals = jnp.exp(scores - log_total)
        probs_bf = prob_vals.astype(jnp.bfloat16)
        attended = jnp.einsum('kgqt,tkd->qkgd', probs_bf.astype(jnp.float32), values_bf.astype(jnp.float32)).astype(jnp.bfloat16)
        attended_flat = attended.reshape(SEQ_LEN, HEADS * HEAD_DIM)
        residual_mid = inputs + jnp.dot(attended_flat, out_proj, preferred_element_type=jnp.float32)
        ffn_normed, unit_two, inv_two = norm_forward(residual_mid, ffn_norm)
        ffn_in = ffn_normed.astype(jnp.bfloat16)
        gate_vals = jnp.dot(ffn_in, gate_proj, preferred_element_type=jnp.float32)
        up_vals = jnp.dot(ffn_in, up_proj, preferred_element_type=jnp.float32)
        sigmoid_gate = jax.nn.sigmoid(gate_vals)
        hidden_act = (gate_vals * sigmoid_gate * up_vals).astype(jnp.bfloat16)
        block_out = (residual_mid + jnp.dot(hidden_act, down_proj, preferred_element_type=jnp.float32)).astype(jnp.bfloat16)
        grad_hidden = jnp.dot(seq_cot, down_proj.T, preferred_element_type=jnp.float32)
        down_grad = jnp.dot(hidden_act.T, seq_cot, preferred_element_type=jnp.float32)
        grad_up = (grad_hidden * (gate_vals * sigmoid_gate)).astype(jnp.bfloat16)
        grad_gate = (grad_hidden * up_vals * sigmoid_gate * (1.0 + gate_vals * (1.0 - sigmoid_gate))).astype(jnp.bfloat16)
        gate_grad = jnp.dot(ffn_in.T, grad_gate, preferred_element_type=jnp.float32)
        up_grad = jnp.dot(ffn_in.T, grad_up, preferred_element_type=jnp.float32)
        grad_ffn_in = jnp.dot(grad_gate, gate_proj.T, preferred_element_type=jnp.float32) + jnp.dot(grad_up, up_proj.T, preferred_element_type=jnp.float32)
        grad_part, ffn_gain_grad = norm_backward(grad_ffn_in, unit_two, inv_two, ffn_norm)
        grad_mid = seq_cot.astype(jnp.float32) + grad_part
        grad_mid_bf = grad_mid.astype(jnp.bfloat16)
        out_grad = jnp.dot(attended_flat.T, grad_mid_bf, preferred_element_type=jnp.float32)
        grad_attended = jnp.dot(grad_mid_bf, out_proj.T, preferred_element_type=jnp.float32).astype(jnp.bfloat16)
        grad_attended = grad_attended.reshape(SEQ_LEN, KV_HEADS, groups, HEAD_DIM)
        delta = lax.optimization_barrier(jnp.sum(grad_attended.astype(jnp.float32) * attended.astype(jnp.float32), axis=-1))
        delta = jnp.transpose(delta, (1, 2, 0))[..., None]
        grad_probs = jnp.einsum('qkgd,tkd->kgqt', grad_attended.astype(jnp.float32), values_bf.astype(jnp.float32))
        grad_scores = (prob_vals * (grad_probs - delta) * score_scale).astype(jnp.bfloat16)
        grad_query_rot = jnp.einsum('kgqt,tkd->qkgd', grad_scores.astype(jnp.float32), key_rot.astype(jnp.float32)).reshape(SEQ_LEN, HEADS, HEAD_DIM)
        grad_key_rot = jnp.einsum('kgqt,qkgd->tkd', grad_scores.astype(jnp.float32), query_rot.astype(jnp.float32))
        grad_vals = jnp.einsum('kgqt,qkgd->tkd', probs_bf.astype(jnp.float32), grad_attended.astype(jnp.float32))
        grad_query_normed = grad_query_rot * cosine_table + rotate_back(grad_query_rot * sine_table)
        grad_key_normed = grad_key_rot * cosine_table + rotate_back(grad_key_rot * sine_table)
        grad_queries, query_gain_grad = norm_backward(grad_query_normed, query_unit, query_inv, query_norm)
        grad_keys, key_gain_grad = norm_backward(grad_key_normed, key_unit, key_inv, key_norm)
        grad_queries_bf = grad_queries.reshape(SEQ_LEN, HEADS * HEAD_DIM).astype(jnp.bfloat16)
        grad_keys_bf = grad_keys.reshape(SEQ_LEN, KV_HEADS * HEAD_DIM).astype(jnp.bfloat16)
        grad_vals_bf = grad_vals.reshape(SEQ_LEN, KV_HEADS * HEAD_DIM).astype(jnp.bfloat16)
        query_grad = jnp.dot(normed_bf.T, grad_queries_bf, preferred_element_type=jnp.float32)
        key_grad = jnp.dot(normed_bf.T, grad_keys_bf, preferred_element_type=jnp.float32)
        value_grad = jnp.dot(normed_bf.T, grad_vals_bf, preferred_element_type=jnp.float32)
        grad_normed_in = jnp.dot(grad_queries_bf, query_proj.T, preferred_element_type=jnp.float32)
        grad_normed_in = grad_normed_in + jnp.dot(grad_keys_bf, key_proj.T, preferred_element_type=jnp.float32)
        grad_normed_in = grad_normed_in + jnp.dot(grad_vals_bf, value_proj.T, preferred_element_type=jnp.float32)
        grad_first, attn_gain_grad = norm_backward(grad_normed_in, unit_one, inv_one, attn_norm)
        input_grad = (grad_mid + grad_first).astype(jnp.bfloat16)
        updates = (query_grad, key_grad, value_grad, out_grad, gate_grad, up_grad, down_grad, attn_gain_grad, query_gain_grad, key_gain_grad, ffn_gain_grad)
        totals = tuple((total_one + update_one for total_one, update_one in zip(totals, updates)))
        return (totals, (block_out, input_grad))
    start_totals = (jnp.zeros(query_proj.shape, jnp.float32), jnp.zeros(key_proj.shape, jnp.float32), jnp.zeros(value_proj.shape, jnp.float32), jnp.zeros(out_proj.shape, jnp.float32), jnp.zeros(gate_proj.shape, jnp.float32), jnp.zeros(up_proj.shape, jnp.float32), jnp.zeros(down_proj.shape, jnp.float32), jnp.zeros(attn_norm.shape, jnp.float32), jnp.zeros(query_norm.shape, jnp.float32), jnp.zeros(key_norm.shape, jnp.float32), jnp.zeros(ffn_norm.shape, jnp.float32))
    sequences = TOKENS // SEQ_LEN
    totals, outputs = lax.scan(one_sequence, start_totals, (hidden_in.reshape(sequences, SEQ_LEN, D), cotangent.reshape(sequences, SEQ_LEN, D)))
    hidden_out = outputs[0].reshape(TOKENS, D)
    dhidden_in = outputs[1].reshape(TOKENS, D)
    return (hidden_out, dhidden_in, totals[0], totals[1], totals[2], totals[3], totals[4], totals[5], totals[6], totals[7], totals[8], totals[9], totals[10])
```

```python
import functools
import math

import jax
import jax.numpy as jnp
from jax import lax
from jax.experimental import pallas as pl
from jax.experimental.pallas import tpu as pltpu
from jax.sharding import PartitionSpec as P

HEAD_DIM = 128
SEQ_LEN = 1024


EPSILON = 1e-06
ROPE_BASE = 1000000.0
NEG_FILL = -1e30


def norm_forward(values, gain):
    inverse = lax.rsqrt(jnp.mean(values * values, axis=-1, keepdims=True) + EPSILON)
    unit_vals = values * inverse
    return (unit_vals * gain, unit_vals, inverse)


def norm_backward(grad_normed, unit_vals, inverse, gain):
    grad_unit = grad_normed * gain
    grad_values = inverse * (
        grad_unit - unit_vals * jnp.mean(grad_unit * unit_vals, axis=-1, keepdims=True)
    )
    grad_gain = jnp.sum((grad_normed * unit_vals).reshape(-1, gain.shape[0]), axis=0)
    return (grad_values, grad_gain)


def rope_tables(positions, width):
    half_width = width // 2
    freqs = ROPE_BASE ** (-(jnp.arange(half_width, dtype=jnp.float32) * (2.0 / width)))
    angles = positions.astype(jnp.float32)[:, None] * freqs[None, :]
    angles = jnp.concatenate([angles, angles], axis=1)
    return (jnp.cos(angles), jnp.sin(angles))


def rotate_half(values):
    half_width = values.shape[-1] // 2
    return jnp.concatenate([-values[..., half_width:], values[..., :half_width]], axis=-1)


def rotate_back(values):
    half_width = values.shape[-1] // 2
    return jnp.concatenate([values[..., half_width:], -values[..., :half_width]], axis=-1)


def masked_scores(query_part, key_rot, offset, score_scale):
    length = key_rot.shape[0]
    q_block = query_part.shape[0]
    scores = (
        jnp.einsum("qkgd,tkd->kgqt", query_part, key_rot, preferred_element_type=jnp.float32)
        * score_scale
    )
    query_pos = offset + jnp.arange(q_block)
    key_pos = jnp.arange(length)
    return jnp.where(key_pos[None, :] <= query_pos[:, None], scores, NEG_FILL)


def attend_forward(query_rot, key_rot, values_bf, score_scale):
    length = query_rot.shape[0]
    q_block = min(512, length)
    attended_parts = []
    total_parts = []
    for offset in range(0, length, q_block):
        scores = masked_scores(query_rot[offset : offset + q_block], key_rot, offset, score_scale)
        top_score = jnp.max(scores, axis=-1, keepdims=True)
        log_total = top_score + jnp.log(
            jnp.sum(jnp.exp(scores - top_score), axis=-1, keepdims=True)
        )
        probs_bf = jnp.exp(scores - log_total).astype(jnp.bfloat16)
        attended_parts.append(
            jnp.einsum(
                "kgqt,tkd->qkgd", probs_bf, values_bf, preferred_element_type=jnp.float32
            ).astype(jnp.bfloat16)
        )
        total_parts.append(log_total)
    return (jnp.concatenate(attended_parts, axis=0), jnp.concatenate(total_parts, axis=2))


def attend_backward(query_rot, key_rot, values_bf, attended, grad_attended, log_total, score_scale):
    length = query_rot.shape[0]
    q_block = min(512, length)
    grad_keys = jnp.zeros(key_rot.shape, jnp.float32)
    grad_vals = jnp.zeros(values_bf.shape, jnp.float32)
    query_parts = []
    for offset in range(0, length, q_block):
        query_part = query_rot[offset : offset + q_block]
        grad_part = grad_attended[offset : offset + q_block]
        scores = masked_scores(query_part, key_rot, offset, score_scale)
        prob_vals = jnp.exp(scores - log_total[:, :, offset : offset + q_block])
        grad_vals = grad_vals + jnp.einsum(
            "kgqt,qkgd->tkd",
            prob_vals.astype(jnp.bfloat16),
            grad_part,
            preferred_element_type=jnp.float32,
        )
        grad_probs = jnp.einsum(
            "qkgd,tkd->kgqt", grad_part, values_bf, preferred_element_type=jnp.float32
        )
        delta = jnp.sum(
            grad_part.astype(jnp.float32) * attended[offset : offset + q_block].astype(jnp.float32),
            axis=-1,
        )
        delta = jnp.transpose(delta, (1, 2, 0))[..., None]
        grad_scores = (prob_vals * (grad_probs - delta) * score_scale).astype(jnp.bfloat16)
        query_parts.append(
            jnp.einsum("kgqt,tkd->qkgd", grad_scores, key_rot, preferred_element_type=jnp.float32)
        )
        grad_keys = grad_keys + jnp.einsum(
            "kgqt,qkgd->tkd", grad_scores, query_part, preferred_element_type=jnp.float32
        )
    return (jnp.concatenate(query_parts, axis=0), grad_keys, grad_vals)


MESH = pl.DeviceIdType.MESH
VMEM_BYTES = 60 * 2**20


def line_barrier(here, count):
    barrier = pltpu.get_barrier_semaphore()

    @pl.when(here > 0)
    def _():
        pl.semaphore_signal(
            barrier, inc=1, device_id={"tensor": here - 1}, device_id_type=MESH
        )

    @pl.when(here < count - 1)
    def _():
        pl.semaphore_signal(
            barrier, inc=1, device_id={"tensor": here + 1}, device_id_type=MESH
        )

    inside = jnp.logical_and(here > 0, here < count - 1)

    @pl.when(inside)
    def _():
        pl.semaphore_wait(barrier, 2)

    @pl.when(jnp.logical_not(inside))
    def _():
        pl.semaphore_wait(barrier, 1)


def block_of(ref, index, rows):
    return ref.at[pl.ds(pl.multiple_of(index * rows, rows), rows)]


class LineGather:
    def __init__(self, here, count, rows, full, send_right, send_left, recv):
        self.here, self.count, self.rows = here, count, rows
        self.full, self.send_right, self.send_left, self.recv = full, send_right, send_left, recv

    def copy(self, index, step, sems, src=None):
        block = block_of(self.full, index, self.rows)
        return pltpu.make_async_remote_copy(
            src_ref=block if src is None else src,
            dst_ref=block,
            send_sem=sems.at[index],
            recv_sem=self.recv.at[index],
            device_id={"tensor": self.here + step},
            device_id_type=MESH,
        )

    def begin(self, own):
        @pl.when(self.here < self.count - 1)
        def _():
            self.copy(self.here, 1, self.send_right, own).start()

        @pl.when(self.here > 0)
        def _():
            self.copy(self.here, -1, self.send_left, own).start()

    def arrive(self, hop, then):
        here, count = self.here, self.count

        @pl.when(here >= hop)
        def _():
            index = here - hop
            self.copy(index, 1, self.send_right).wait_recv()

            @pl.when(here < count - 1)
            def _():
                self.copy(index, 1, self.send_right).start()

        @pl.when(here < count - hop)
        def _():
            index = here + hop
            self.copy(index, -1, self.send_left).wait_recv()

            @pl.when(here > 0)
            def _():
                self.copy(index, -1, self.send_left).start()

        @pl.when(here >= hop)
        def _():
            then(here - hop)

        @pl.when(here < count - hop)
        def _():
            then(here + hop)

    def finish(self):
        here, count = self.here, self.count
        for hop in range(count):

            @pl.when(jnp.logical_and(here >= hop, here < count - 1))
            def _():
                self.copy(here - hop, 1, self.send_right).wait_send()

            @pl.when(jnp.logical_and(here < count - hop, here > 0))
            def _():
                self.copy(here + hop, -1, self.send_left).wait_send()


class LineScatter:
    def __init__(self, here, count, from_left, from_right, to_right, to_left, sems):
        self.here, self.count = here, count
        self.from_left, self.from_right = from_left, from_right
        self.to_right, self.to_left = to_right, to_left
        self.sems = sems

    def right(self, index):
        return pltpu.make_async_remote_copy(
            src_ref=self.to_right.at[index],
            dst_ref=self.from_left.at[index],
            send_sem=self.sems.at[0, index],
            recv_sem=self.sems.at[1, index],
            device_id={"tensor": self.here + 1},
            device_id_type=MESH,
        )

    def left(self, index):
        return pltpu.make_async_remote_copy(
            src_ref=self.to_left.at[index],
            dst_ref=self.from_right.at[index],
            send_sem=self.sems.at[2, index],
            recv_sem=self.sems.at[3, index],
            device_id={"tensor": self.here - 1},
            device_id_type=MESH,
        )

    def step(self, hop, part):
        here, count = self.here, self.count

        @pl.when(jnp.logical_and(hop >= here, here < count - 1))
        def _():
            index = count - 1 + here - hop

            @pl.when(here > 0)
            def _():
                self.right(index).wait_recv()
                self.to_right[index] = (
                    part(index).astype(jnp.float32)
                    + self.from_left[index].astype(jnp.float32)
                ).astype(jnp.bfloat16)

            @pl.when(here == 0)
            def _():
                self.to_right[index] = part(index)

            self.right(index).start()

        @pl.when(jnp.logical_and(hop >= count - 1 - here, here > 0))
        def _():
            index = hop + here + 1 - count

            @pl.when(here < count - 1)
            def _():
                self.left(index).wait_recv()
                self.to_left[index] = (
                    part(index).astype(jnp.float32)
                    + self.from_right[index].astype(jnp.float32)
                ).astype(jnp.bfloat16)

            @pl.when(here == count - 1)
            def _():
                self.to_left[index] = part(index)

            self.left(index).start()

    def finish(self, own, store):
        here, count = self.here, self.count

        @pl.when(here > 0)
        def _():
            self.right(here).wait_recv()

        @pl.when(here < count - 1)
        def _():
            self.left(here).wait_recv()

        @pl.when(here == 0)
        def _():
            store(own() + self.from_right[here].astype(jnp.float32))

        @pl.when(here == count - 1)
        def _():
            store(own() + self.from_left[here].astype(jnp.float32))

        @pl.when(jnp.logical_and(here > 0, here < count - 1))
        def _():
            store(
                own()
                + self.from_left[here].astype(jnp.float32)
                + self.from_right[here].astype(jnp.float32)
            )

        for hop in range(count - 1):

            @pl.when(jnp.logical_and(hop >= here, here < count - 1))
            def _():
                self.right(count - 1 + here - hop).wait_send()

            @pl.when(jnp.logical_and(hop >= count - 1 - here, here > 0))
            def _():
                self.left(hop + here + 1 - count).wait_send()


def gather_kernel(count, x_ref, out_ref, full, send_right, send_left, recv, done):
    here = lax.axis_index("tensor")
    rows = x_ref.shape[0]
    line_barrier(here, count)
    line = LineGather(here, count, rows, full, send_right, send_left, recv)
    line.begin(x_ref)

    def put(index):
        return pltpu.make_async_copy(
            block_of(full, index, rows), block_of(out_ref, index, rows), done.at[index]
        )

    own = pltpu.make_async_copy(x_ref, block_of(out_ref, here, rows), done.at[here])
    own.start()
    for hop in range(1, count):
        line.arrive(hop, lambda index: put(index).start())
    own.wait()
    for index in range(count):

        @pl.when(index != here)
        def _():
            put(index).wait()

    line.finish()


def line_gather(x, collective):
    count = lax.axis_size("tensor")
    rows, width = x.shape
    return pl.pallas_call(
        functools.partial(gather_kernel, count),
        out_shape=jax.ShapeDtypeStruct((count * rows, width), x.dtype),
        in_specs=[pl.BlockSpec(memory_space=pltpu.VMEM)],
        out_specs=pl.BlockSpec(memory_space=pl.ANY),
        scratch_shapes=[
            pltpu.VMEM((count * rows, width), x.dtype),
            pltpu.SemaphoreType.DMA((count,)),
            pltpu.SemaphoreType.DMA((count,)),
            pltpu.SemaphoreType.DMA((count,)),
            pltpu.SemaphoreType.DMA((count,)),
        ],
        compiler_params=pltpu.CompilerParams(
            collective_id=collective, has_side_effects=True, vmem_limit_bytes=VMEM_BYTES
        ),
        cost_estimate=pl.CostEstimate(
            flops=0, transcendentals=0, bytes_accessed=64 * count * rows * width
        ),
    )(x)


def scatter_kernel(
    count, part_ref, out_ref, part, from_left, from_right, to_right, to_left, sems, got
):
    here = lax.axis_index("tensor")
    rows = part.shape[1]
    line_barrier(here, count)
    line = LineScatter(here, count, from_left, from_right, to_right, to_left, sems)

    def fetch(index):
        return pltpu.make_async_copy(block_of(part_ref, index, rows), part.at[index], got.at[index])

    for index in range(count):
        fetch(index).start()
    for index in range(count):
        fetch(index).wait()
    for hop in range(count - 1):
        line.step(hop, lambda index: part[index])

    def store(total):
        out_ref[...] = total

    line.finish(lambda: part[here].astype(jnp.float32), store)


def line_scatter(parts, collective):
    count = lax.axis_size("tensor")
    rows, width = parts.shape[0] // count, parts.shape[1]
    block = (count, rows, width)
    return pl.pallas_call(
        functools.partial(scatter_kernel, count),
        out_shape=jax.ShapeDtypeStruct((rows, width), jnp.float32),
        in_specs=[pl.BlockSpec(memory_space=pl.ANY)],
        out_specs=pl.BlockSpec(memory_space=pltpu.VMEM),
        scratch_shapes=[pltpu.VMEM(block, jnp.bfloat16)] * 5
        + [pltpu.SemaphoreType.DMA((4, count)), pltpu.SemaphoreType.DMA((count,))],
        compiler_params=pltpu.CompilerParams(
            collective_id=collective, has_side_effects=True, vmem_limit_bytes=VMEM_BYTES
        ),
        cost_estimate=pl.CostEstimate(
            flops=0, transcendentals=0, bytes_accessed=64 * count * rows * width
        ),
    )(parts)


def total_kernel(line, planes, x_ref, out_ref, slots, send, recv):
    plane, here = lax.axis_index("dp"), lax.axis_index("tensor")
    me, everyone = plane * line + here, line * planes
    barrier = pltpu.get_barrier_semaphore()

    def greet(index, carry):
        @pl.when(index != me)
        def _():
            pl.semaphore_signal(
                barrier, inc=1, device_id=(index // line, index % line), device_id_type=MESH
            )

        return carry

    lax.fori_loop(0, everyone, greet, 0)
    pl.semaphore_wait(barrier, everyone - 1)

    def to(index):
        return pltpu.make_async_remote_copy(
            src_ref=x_ref,
            dst_ref=slots.at[me],
            send_sem=send.at[index],
            recv_sem=recv.at[me],
            device_id=(index // line, index % line),
            device_id_type=MESH,
        )

    def came(index):
        return pltpu.make_async_remote_copy(
            src_ref=x_ref,
            dst_ref=slots.at[index],
            send_sem=send.at[index],
            recv_sem=recv.at[index],
            device_id=(index // line, index % line),
            device_id_type=MESH,
        )

    def push(index, carry):
        @pl.when(index != me)
        def _():
            to(index).start()

        return carry

    lax.fori_loop(0, everyone, push, 0)
    slots[me] = x_ref[...]

    def settle(index, carry):
        @pl.when(index != me)
        def _():
            came(index).wait_recv()
            to(index).wait_send()

        return carry

    lax.fori_loop(0, everyone, settle, 0)

    def add(index, total):
        return total + slots[index]

    out_ref[...] = lax.fori_loop(0, everyone, add, jnp.zeros(x_ref.shape, jnp.float32))


def total_over_all(x, collective):
    line, planes = lax.axis_size("tensor"), lax.axis_size("dp")
    return pl.pallas_call(
        functools.partial(total_kernel, line, planes),
        out_shape=jax.ShapeDtypeStruct(x.shape, x.dtype),
        in_specs=[pl.BlockSpec(memory_space=pltpu.VMEM)],
        out_specs=pl.BlockSpec(memory_space=pltpu.VMEM),
        scratch_shapes=[
            pltpu.VMEM((line * planes,) + x.shape, x.dtype),
            pltpu.SemaphoreType.DMA((line * planes,)),
            pltpu.SemaphoreType.DMA((line * planes,)),
        ],
        compiler_params=pltpu.CompilerParams(collective_id=collective, has_side_effects=True),
    )(x)


def matmul(left, right, dims):
    return lax.dot_general(left, right, (dims, ((), ())), preferred_element_type=jnp.float32)


def over_sequences(function, operands):
    if operands[0].shape[0] == 1:
        results = function(tuple(operand[0] for operand in operands))
        return tuple(result[None] for result in results)
    return lax.map(function, operands)


def per_device(
    hidden_in,
    query_proj,
    key_proj,
    value_proj,
    out_proj,
    gate_proj,
    up_proj,
    down_proj,
    attn_norm,
    query_norm,
    key_norm,
    ffn_norm,
    cotangent,
):
    heads_width, kv_width, hidden_width = query_proj.shape[1], key_proj.shape[1], gate_proj.shape[1]
    attn_full = lax.all_gather(
        jnp.concatenate([query_proj, key_proj, value_proj, out_proj.T], axis=1),
        "dp",
        axis=0,
        tiled=True,
    )
    gate_up_full = lax.all_gather(
        jnp.concatenate([gate_proj, up_proj], axis=1), "dp", axis=0, tiled=True
    )
    down_full_t = lax.all_gather(down_proj.T, "dp", axis=0, tiled=True)
    query_full, key_full, value_full, out_full_t = jnp.split(
        attn_full, [heads_width, heads_width + kv_width, heads_width + 2 * kv_width], axis=1
    )
    gate_full, up_full = jnp.split(gate_up_full, 2, axis=1)
    local_rows = hidden_in.shape[0]
    score_scale = 1.0 / math.sqrt(HEAD_DIM)
    inputs = hidden_in.astype(jnp.float32)
    normed, unit_one, inv_one = norm_forward(inputs, attn_norm)
    normed_bf = line_gather(normed.astype(jnp.bfloat16), 0)
    group_rows = normed_bf.shape[0]
    local_heads = query_full.shape[1] // HEAD_DIM
    local_kv = key_full.shape[1] // HEAD_DIM
    groups = local_heads // local_kv
    sequences = group_rows // SEQ_LEN
    queries = jnp.dot(normed_bf, query_full, preferred_element_type=jnp.float32).reshape(
        group_rows, local_heads, HEAD_DIM
    )
    keys_raw = jnp.dot(normed_bf, key_full, preferred_element_type=jnp.float32).reshape(
        group_rows, local_kv, HEAD_DIM
    )
    values_bf = jnp.dot(normed_bf, value_full, preferred_element_type=jnp.float32).astype(
        jnp.bfloat16
    )
    values_bf = values_bf.reshape(sequences, SEQ_LEN, local_kv, HEAD_DIM)
    query_normed, query_unit, query_inv = norm_forward(queries, query_norm)
    key_normed, key_unit, key_inv = norm_forward(keys_raw, key_norm)
    cosine_table, sine_table = rope_tables(jnp.arange(group_rows) % SEQ_LEN, HEAD_DIM)
    cosine_table = cosine_table[:, None, :]
    sine_table = sine_table[:, None, :]
    query_rot = (query_normed * cosine_table + rotate_half(query_normed) * sine_table).astype(
        jnp.bfloat16
    )
    query_rot = query_rot.reshape(sequences, SEQ_LEN, local_kv, groups, HEAD_DIM)
    key_rot = (key_normed * cosine_table + rotate_half(key_normed) * sine_table).astype(
        jnp.bfloat16
    )
    key_rot = key_rot.reshape(sequences, SEQ_LEN, local_kv, HEAD_DIM)
    attended, log_total = over_sequences(
        lambda packed: attend_forward(packed[0], packed[1], packed[2], score_scale),
        (query_rot, key_rot, values_bf),
    )
    attended_flat = attended.reshape(group_rows, local_heads * HEAD_DIM)
    residual_mid = inputs + line_scatter(
        matmul(attended_flat, out_full_t, ((1,), (1,))).astype(jnp.bfloat16), 1
    )
    ffn_normed, unit_two, inv_two = norm_forward(residual_mid, ffn_norm)
    ffn_in = line_gather(ffn_normed.astype(jnp.bfloat16), 2)
    gate_vals = jnp.dot(ffn_in, gate_full, preferred_element_type=jnp.float32)
    up_vals = jnp.dot(ffn_in, up_full, preferred_element_type=jnp.float32)
    sigmoid_gate = jax.nn.sigmoid(gate_vals)
    hidden_act = (gate_vals * sigmoid_gate * up_vals).astype(jnp.bfloat16)
    hidden_out = (
        residual_mid
        + line_scatter(matmul(hidden_act, down_full_t, ((1,), (1,))).astype(jnp.bfloat16), 3)
    ).astype(jnp.bfloat16)
    cot_full = line_gather(cotangent, 4)
    grad_hidden = jnp.dot(cot_full, down_full_t, preferred_element_type=jnp.float32)
    down_grad_t = matmul(cot_full, hidden_act, ((0,), (0,)))
    grad_up = (grad_hidden * (gate_vals * sigmoid_gate)).astype(jnp.bfloat16)
    grad_gate = (
        grad_hidden * up_vals * sigmoid_gate * (1.0 + gate_vals * (1.0 - sigmoid_gate))
    ).astype(jnp.bfloat16)
    gate_grad = jnp.dot(ffn_in.T, grad_gate, preferred_element_type=jnp.float32)
    up_grad = jnp.dot(ffn_in.T, grad_up, preferred_element_type=jnp.float32)
    total = jnp.dot(grad_gate, gate_full.T, preferred_element_type=jnp.float32)
    total = total + jnp.dot(grad_up, up_full.T, preferred_element_type=jnp.float32)
    grad_ffn_in = line_scatter(total.astype(jnp.bfloat16), 5)
    grad_part, ffn_gain_grad = norm_backward(grad_ffn_in, unit_two, inv_two, ffn_norm)
    grad_mid = cotangent.astype(jnp.float32) + grad_part
    grad_mid_bf = line_gather(grad_mid.astype(jnp.bfloat16), 6)
    out_grad_t = matmul(grad_mid_bf, attended_flat, ((0,), (0,)))
    grad_attended = jnp.dot(grad_mid_bf, out_full_t, preferred_element_type=jnp.float32).astype(
        jnp.bfloat16
    )
    grad_attended = grad_attended.reshape(sequences, SEQ_LEN, local_kv, groups, HEAD_DIM)
    grad_query_rot, grad_key_rot, grad_vals = over_sequences(
        lambda packed: attend_backward(
            packed[0], packed[1], packed[2], packed[3], packed[4], packed[5], score_scale
        ),
        (query_rot, key_rot, values_bf, attended, grad_attended, log_total),
    )
    grad_query_rot = grad_query_rot.reshape(group_rows, local_heads, HEAD_DIM)
    grad_key_rot = grad_key_rot.reshape(group_rows, local_kv, HEAD_DIM)
    grad_query_normed = grad_query_rot * cosine_table + rotate_back(grad_query_rot * sine_table)
    grad_key_normed = grad_key_rot * cosine_table + rotate_back(grad_key_rot * sine_table)
    grad_queries, query_gain_grad = norm_backward(
        grad_query_normed, query_unit, query_inv, query_norm
    )
    grad_keys, key_gain_grad = norm_backward(grad_key_normed, key_unit, key_inv, key_norm)
    grad_queries_bf = grad_queries.reshape(group_rows, local_heads * HEAD_DIM).astype(jnp.bfloat16)
    grad_keys_bf = grad_keys.reshape(group_rows, local_kv * HEAD_DIM).astype(jnp.bfloat16)
    grad_vals_bf = grad_vals.reshape(group_rows, local_kv * HEAD_DIM).astype(jnp.bfloat16)
    query_grad = jnp.dot(normed_bf.T, grad_queries_bf, preferred_element_type=jnp.float32)
    key_grad = jnp.dot(normed_bf.T, grad_keys_bf, preferred_element_type=jnp.float32)
    value_grad = jnp.dot(normed_bf.T, grad_vals_bf, preferred_element_type=jnp.float32)
    total = jnp.dot(grad_queries_bf, query_full.T, preferred_element_type=jnp.float32)
    total = total + jnp.dot(grad_keys_bf, key_full.T, preferred_element_type=jnp.float32)
    total = total + jnp.dot(grad_vals_bf, value_full.T, preferred_element_type=jnp.float32)
    grad_normed_in = line_scatter(total.astype(jnp.bfloat16), 7)
    grad_first, attn_gain_grad = norm_backward(grad_normed_in, unit_one, inv_one, attn_norm)
    dhidden_in = (grad_mid + grad_first).astype(jnp.bfloat16)
    gains = (attn_gain_grad, query_gain_grad, key_gain_grad, ffn_gain_grad)
    lengths = [gain.shape[0] for gain in gains]
    packed = jnp.concatenate(gains)
    gain_total = total_over_all(packed.reshape(-1, HEAD_DIM), 8).reshape(-1)
    gain_totals = jnp.split(gain_total, [sum(lengths[:k]) for k in range(1, len(lengths))])

    def scatter(parts):
        return lax.psum_scatter(
            jnp.concatenate([part.astype(jnp.bfloat16) for part in parts], axis=1),
            "dp",
            scatter_dimension=0,
            tiled=True,
        ).astype(jnp.float32)

    down_sum_t = scatter([down_grad_t])
    gate_sum, up_sum = jnp.split(scatter([gate_grad, up_grad]), 2, axis=1)
    query_sum, key_sum, value_sum, out_sum_t = jnp.split(
        scatter([query_grad, key_grad, value_grad, out_grad_t]),
        [heads_width, heads_width + kv_width, heads_width + 2 * kv_width],
        axis=1,
    )
    weight_sums = (query_sum, key_sum, value_sum, out_sum_t.T, gate_sum, up_sum, down_sum_t.T)
    return (
        hidden_out,
        dhidden_in,
        weight_sums[0],
        weight_sums[1],
        weight_sums[2],
        weight_sums[3],
        weight_sums[4],
        weight_sums[5],
        weight_sums[6],
        gain_totals[0],
        gain_totals[1],
        gain_totals[2],
        gain_totals[3],
    )


def solution(mesh):
    placed = (
        P(("dp", "tensor"), None),
        P("dp", "tensor"),
        P("dp", "tensor"),
        P("dp", "tensor"),
        P("tensor", "dp"),
        P("dp", "tensor"),
        P("dp", "tensor"),
        P("tensor", "dp"),
        P(),
        P(),
        P(),
        P(),
        P(("dp", "tensor"), None),
    )
    return jax.shard_map(
        per_device,
        mesh=mesh,
        in_specs=placed,
        out_specs=(
            P(("dp", "tensor"), None),
            P(("dp", "tensor"), None),
            P("dp", "tensor"),
            P("dp", "tensor"),
            P("dp", "tensor"),
            P("tensor", "dp"),
            P("dp", "tensor"),
            P("dp", "tensor"),
            P("tensor", "dp"),
            P(),
            P(),
            P(),
            P(),
        ),
        check_vma=False,
    )
```

```python
import functools
import math

import jax
import jax.numpy as jnp
from jax import lax
from jax.experimental import pallas as pl
from jax.experimental.pallas import tpu as pltpu
from jax.sharding import PartitionSpec as P

HEAD_DIM = 128
SEQ_LEN = 1024


EPSILON = 1e-06
ROPE_BASE = 1000000.0
NEG_FILL = -1e30
MESH = pl.DeviceIdType.MESH
VMEM_BYTES = 63 * 2**20
TILE = 512
F32, BF16 = jnp.float32, jnp.bfloat16
NN, NT, TN = ((1,), (0,)), ((1,), (1,)), ((0,), (0,))
IN_VMEM, IN_HBM = pl.BlockSpec(memory_space=pltpu.VMEM), pl.BlockSpec(memory_space=pl.ANY)
DMA = pltpu.SemaphoreType.DMA


def matmul(left, right, dims):
    return lax.dot_general(left, right, (dims, ((), ())), preferred_element_type=F32)


def tile_of(size):
    return TILE if size % TILE == 0 else size


def span(index, size):
    return pl.ds(pl.multiple_of(index * size, size), size)


def loop(start, stop, body):
    lax.fori_loop(start, stop, lambda index, carry: (body(index), carry)[1], 0)


def params(collective=None):
    return pltpu.CompilerParams(
        collective_id=collective, has_side_effects=True, vmem_limit_bytes=VMEM_BYTES
    )


def greet_line(here, count):
    barrier = pltpu.get_barrier_semaphore()

    @pl.when(here > 0)
    def _():
        pl.semaphore_signal(barrier, inc=1, device_id={"tensor": here - 1}, device_id_type=MESH)

    @pl.when(here < count - 1)
    def _():
        pl.semaphore_signal(barrier, inc=1, device_id={"tensor": here + 1}, device_id_type=MESH)


def meet_line(here, count):
    barrier = pltpu.get_barrier_semaphore()
    inside = jnp.logical_and(here > 0, here < count - 1)

    @pl.when(inside)
    def _():
        pl.semaphore_wait(barrier, 2)

    @pl.when(jnp.logical_not(inside))
    def _():
        pl.semaphore_wait(barrier, 1)


class LineGather:
    def __init__(self, here, count, rows, full, sems):
        self.here, self.count, self.rows, self.full, self.sems = here, count, rows, full, sems

    def copy(self, index, step, src=None):
        block = self.full.at[span(index, self.rows)]
        return pltpu.make_async_remote_copy(
            src_ref=block if src is None else src,
            dst_ref=block,
            send_sem=self.sems.at[0 if step > 0 else 1, index],
            recv_sem=self.sems.at[2, index],
            device_id={"tensor": self.here + step},
            device_id_type=MESH,
        )

    def begin(self, own=None):
        @pl.when(self.here < self.count - 1)
        def _():
            self.copy(self.here, 1, own).start()

        @pl.when(self.here > 0)
        def _():
            self.copy(self.here, -1, own).start()

    def arrive(self, hop):
        here, count = self.here, self.count

        @pl.when(here >= hop)
        def _():
            self.copy(here - hop, 1).wait_recv()

            @pl.when(here < count - 1)
            def _():
                self.copy(here - hop, 1).start()

        @pl.when(here < count - hop)
        def _():
            self.copy(here + hop, -1).wait_recv()

            @pl.when(here > 0)
            def _():
                self.copy(here + hop, -1).start()

    def each(self, hop, then):
        def side(which):
            index = self.here + (2 * which - 1) * hop
            fits = jnp.logical_and(index >= 0, index < self.count)

            @pl.when(jnp.logical_and(fits, which + hop > 0))
            def _():
                then(index)

        loop(0, 2, side)

    def finish(self):
        here, count = self.here, self.count

        def settle(hop):
            @pl.when(jnp.logical_and(here >= hop, here < count - 1))
            def _():
                self.copy(here - hop, 1).wait_send()

            @pl.when(jnp.logical_and(here < count - hop, here > 0))
            def _():
                self.copy(here + hop, -1).wait_send()

        loop(0, count, settle)


class LineScatter:
    def __init__(self, here, count, came, going, sems):
        self.here, self.count, self.came, self.going, self.sems = here, count, came, going, sems

    def right(self, index):
        return pltpu.make_async_remote_copy(
            src_ref=self.going.at[index],
            dst_ref=self.came.at[index + 1],
            send_sem=self.sems.at[0, index],
            recv_sem=self.sems.at[1, index],
            device_id={"tensor": self.here + 1},
            device_id_type=MESH,
        )

    def left(self, index):
        return pltpu.make_async_remote_copy(
            src_ref=self.going.at[index],
            dst_ref=self.came.at[index],
            send_sem=self.sems.at[2, index],
            recv_sem=self.sems.at[3, index],
            device_id={"tensor": self.here - 1},
            device_id_type=MESH,
        )

    def goes_right(self, hop):
        return jnp.logical_and(hop >= self.here, self.here < self.count - 1)

    def goes_left(self, hop):
        return jnp.logical_and(hop >= self.count - 1 - self.here, self.here > 0)

    def rightward(self, hop):
        return self.count - 1 + self.here - hop

    def leftward(self, hop):
        return hop + self.here + 1 - self.count

    def each(self, hop, then):
        def side(which):
            goes = jnp.where(which == 0, self.goes_right(hop), self.goes_left(hop))

            @pl.when(goes)
            def _():
                then((1 - which) * self.rightward(hop) + which * self.leftward(hop))

        loop(0, 2, side)

    def add(self, index, slot):
        self.going[index] = (
            self.going[index].astype(F32) + self.came[slot].astype(F32)
        ).astype(BF16)

    def step(self, hop):
        here, count = self.here, self.count

        @pl.when(self.goes_right(hop))
        def _():
            index = self.rightward(hop)

            @pl.when(here > 0)
            def _():
                self.right(index).wait_recv()
                self.add(index, index + 1)

            self.right(index).start()

        @pl.when(self.goes_left(hop))
        def _():
            index = self.leftward(hop)

            @pl.when(here < count - 1)
            def _():
                self.left(index).wait_recv()
                self.add(index, index)

            self.left(index).start()

    def finish(self, total):
        here, count = self.here, self.count

        @pl.when(here > 0)
        def _():
            self.right(here).wait_recv()
            total[...] += self.came[here + 1].astype(F32)

        @pl.when(here < count - 1)
        def _():
            self.left(here).wait_recv()
            total[...] += self.came[here].astype(F32)

        def settle(hop):
            @pl.when(self.goes_right(hop))
            def _():
                self.right(self.rightward(hop)).wait_send()

            @pl.when(self.goes_left(hop))
            def _():
                self.left(self.leftward(hop)).wait_send()

        loop(0, count - 1, settle)


def scatter_scratch(count, rows, width):
    return [
        pltpu.VMEM((count + 1, rows, width), BF16),
        pltpu.VMEM((count, rows, width), BF16),
        DMA((4, count)),
    ]


def gather_scratch(count, rows, width):
    return [pltpu.VMEM((count * rows, width), BF16), DMA((3, count))]


def row_blocks(rows):
    return 64 if rows % 64 == 0 else rows


def norm_rows(values_ref, gain_ref, store):
    block = row_blocks(values_ref.shape[0])

    def body(index):
        rows = span(index, block)
        values = values_ref[rows, :].astype(F32)
        inverse = lax.rsqrt(jnp.mean(values * values, axis=-1, keepdims=True) + EPSILON)
        store(rows, values * inverse * gain_ref[...])

    loop(0, values_ref.shape[0] // block, body)


def norm_rows_backward(grad_ref, values_ref, gain_ref, gain_grad_ref, store):
    block = row_blocks(values_ref.shape[0])
    gain_grad_ref[...] = jnp.zeros_like(gain_grad_ref)

    def body(index):
        rows = span(index, block)
        values, grad = values_ref[rows, :].astype(F32), grad_ref[rows, :]
        inverse = lax.rsqrt(jnp.mean(values * values, axis=-1, keepdims=True) + EPSILON)
        unit = values * inverse
        grad_unit = grad * gain_ref[...]
        mean = jnp.mean(grad_unit * unit, axis=-1, keepdims=True)
        gain_grad_ref[...] += jnp.sum(grad * unit, axis=0, keepdims=True)
        store(rows, inverse * (grad_unit - unit * mean))

    loop(0, values_ref.shape[0] // block, body)


def first_kernel(count, hidden_ref, gain_ref, out_ref, full, sems, done):
    here = lax.axis_index("tensor")
    rows = hidden_ref.shape[0]
    greet_line(here, count)
    own = full.at[span(here, rows)]

    def store(block, normed):
        own[block, :] = normed.astype(BF16)

    norm_rows(hidden_ref, gain_ref, store)
    meet_line(here, count)
    line = LineGather(here, count, rows, full, sems)
    line.begin()

    def put(index):
        return pltpu.make_async_copy(
            full.at[span(index, rows)], out_ref.at[span(index, rows)], done.at[index]
        )

    def pass_on(hop):
        @pl.when(hop > 0)
        def _():
            line.arrive(hop)

        line.each(hop, lambda index: put(index).start())

    loop(0, count, pass_on)
    loop(0, count, lambda index: put(index).wait())
    line.finish()


def first_gather(hidden, gain, collective):
    count = lax.axis_size("tensor")
    rows, width = hidden.shape
    return pl.pallas_call(
        functools.partial(first_kernel, count),
        out_shape=jax.ShapeDtypeStruct((count * rows, width), BF16),
        in_specs=[IN_VMEM, IN_VMEM],
        out_specs=IN_HBM,
        scratch_shapes=gather_scratch(count, rows, width) + [DMA((count,))],
        compiler_params=params(collective),
        cost_estimate=pl.CostEstimate(
            flops=0, transcendentals=0, bytes_accessed=64 * count * rows * width
        ),
        name="first_gather",
    )(hidden, gain[None])


def middle_kernel(
    count, attended, weights, hidden_ref, cot_ref, mid_ref, cot_out,
    came, going, scatter_sems, full, gather_sems, done,
):
    here = lax.axis_index("tensor")
    rows, width = hidden_ref.shape
    tile = tile_of(width)
    out_columns = slice(weights.shape[1] - attended.shape[1], weights.shape[1])
    greet_line(here, count)

    def term(index, store):
        left = attended[span(index, rows), :]

        def column(k):
            store(span(k, tile), matmul(left, weights[span(k, tile), out_columns], NT))

        loop(0, width // tile, column)

    def part(index):
        def store(columns, value):
            going[index, :, columns] = value.astype(BF16)

        term(index, store)

    scatter = LineScatter(here, count, came, going, scatter_sems)
    gather = LineGather(here, count, rows, full, gather_sems)

    def put(index):
        return pltpu.make_async_copy(
            full.at[span(index, rows)], cot_out.at[span(index, rows)], done.at[index]
        )

    own = pltpu.make_async_copy(cot_ref, cot_out.at[span(here, rows)], done.at[here])
    own.start()
    scatter.each(0, part)
    meet_line(here, count)
    scatter.step(0)
    gather.begin(cot_ref)

    def own_term(columns, value):
        mid_ref[:, columns] = hidden_ref[:, columns].astype(F32) + value

    term(here, own_term)

    def pass_on(hop):
        scatter.each(hop, part)
        scatter.step(hop)
        gather.arrive(hop)
        gather.each(hop, lambda index: put(index).start())

    loop(1, count - 1, pass_on)
    gather.arrive(count - 1)
    gather.each(count - 1, lambda index: put(index).start())
    scatter.finish(mid_ref)
    own.wait()

    def settle(index):
        @pl.when(index != here)
        def _():
            put(index).wait()

    loop(0, count, settle)
    gather.finish()


def middle_scatter(attended, weights, hidden, cotangent, collective):
    count = lax.axis_size("tensor")
    rows, width = hidden.shape
    return pl.pallas_call(
        functools.partial(middle_kernel, count),
        out_shape=[
            jax.ShapeDtypeStruct((rows, width), F32),
            jax.ShapeDtypeStruct((count * rows, width), BF16),
        ],
        in_specs=[IN_VMEM] * 4,
        out_specs=[IN_VMEM, IN_HBM],
        scratch_shapes=scatter_scratch(count, rows, width)
        + gather_scratch(count, rows, width)
        + [DMA((count,))],
        compiler_params=params(collective),
        cost_estimate=pl.CostEstimate(
            flops=0, transcendentals=0, bytes_accessed=80 * count * rows * width
        ),
        name="middle_scatter",
    )(attended, weights, hidden, cotangent)


def ffn_kernel(
    count, mid_ref, gain_ref, cot_hbm, gate_up_hbm, down_hbm,
    grad_mid, gain_grad, out_part, weight_grad,
    full, gather_sems, came, going, scatter_sems,
    cot, gate_up, down_t, act, grads, stage, loads, stores,
):
    here = lax.axis_index("tensor")
    rows, width = mid_ref.shape
    hidden = down_t.shape[1]
    cols, tile = tile_of(hidden), tile_of(width)
    greet_line(here, count)
    fetches = [
        pltpu.make_async_copy(src, dst, loads.at[k])
        for k, (src, dst) in enumerate(
            ((cot_hbm, cot), (down_hbm, down_t), (gate_up_hbm, gate_up))
        )
    ]
    for fetch in fetches:
        fetch.start()
    own = full.at[span(here, rows)]

    def store_normed(block, normed):
        own[block, :] = normed.astype(BF16)

    norm_rows(mid_ref, gain_ref, store_normed)
    meet_line(here, count)
    gather = LineGather(here, count, rows, full, gather_sems)
    scatter = LineScatter(here, count, came, going, scatter_sems)
    gather.begin()
    fetches[0].wait()
    fetches[1].wait()

    def grad_hidden(index):
        block, columns = span(index // (hidden // cols), rows), span(index % (hidden // cols), cols)
        grads[block, columns] = matmul(cot[block, :], down_t[:, columns], NN).astype(BF16)

    loop(0, count * (hidden // cols), grad_hidden)
    fetches[2].wait()

    def forward(index):
        block = span(index, rows)

        def column(k):
            here_cols, up_cols = span(k, cols), pl.ds(pl.multiple_of(hidden + k * cols, cols), cols)
            gate = matmul(full[block, :], gate_up[:, here_cols], NN)
            up = matmul(full[block, :], gate_up[:, up_cols], NN)
            grad = grads[block, here_cols].astype(F32)
            sigmoid = jax.nn.sigmoid(gate)
            silu = gate * sigmoid
            act[block, here_cols] = (silu * up).astype(BF16)
            grads[block, up_cols] = (grad * silu).astype(BF16)
            grads[block, here_cols] = (
                grad * up * sigmoid * (1.0 + gate * (1.0 - sigmoid))
            ).astype(BF16)

        loop(0, hidden // cols, column)

    def pass_on(hop):
        @pl.when(hop > 0)
        def _():
            gather.arrive(hop)

        gather.each(hop, forward)

    loop(0, count, pass_on)

    def term(index, store):
        block = span(index, rows)

        def column(k):
            store(span(k, tile), matmul(grads[block, :], gate_up[span(k, tile), :], NT))

        loop(0, width // tile, column)

    def part(index):
        def store(columns, value):
            going[index, :, columns] = value.astype(BF16)

        term(index, store)

    def own_term(columns, value):
        grad_mid[:, columns] = value

    def put(slot, target):
        return pltpu.make_async_copy(stage.at[slot], target, stores.at[slot])

    def stream(total, compute, target):
        def body(index):
            slot = index % 2

            @pl.when(index >= 2)
            def _():
                put(slot, target(index - 2)).wait()

            stage[slot] = compute(index).astype(BF16)
            put(slot, target(index)).start()

        loop(0, total, body)
        for index in range(max(0, total - 2), total):
            put(index % 2, target(index)).wait()

    across = width // tile

    def output_tile(index):
        return matmul(
            act[span(index // across, tile), :], down_t[span(index % across, tile), :], NT
        )

    def output_target(index):
        return out_part.at[span(index // across, tile), span(index % across, tile)]

    wide = hidden // cols

    def down_tile(index):
        return matmul(cot[:, span(index // wide, tile)], act[:, span(index % wide, cols)], TN)

    def down_target(index):
        columns = pl.ds(pl.multiple_of((2 * wide + index % wide) * cols, cols), cols)
        return weight_grad.at[span(index // wide, tile), columns]

    def gate_up_tile(index):
        return matmul(
            full[:, span(index // (2 * wide), tile)], grads[:, span(index % (2 * wide), cols)], TN
        )

    def gate_up_target(index):
        return weight_grad.at[span(index // (2 * wide), tile), span(index % (2 * wide), cols)]

    def scatter_hop(hop):
        scatter.each(hop, part)
        scatter.step(hop)

        @pl.when(hop == 0)
        def _():
            term(here, own_term)
            stream(count * rows // tile * across, output_tile, output_target)

        @pl.when(hop == 1)
        def _():
            stream(across * wide, down_tile, down_target)

    loop(0, count - 1, scatter_hop)
    stream(across * 2 * wide, gate_up_tile, gate_up_target)
    scatter.finish(grad_mid)
    gather.finish()

    def store_grad(block, value):
        rows_here = pl.ds(here * rows + block.start, block.size)
        grad_mid[block, :] = cot[rows_here, :].astype(F32) + value

    norm_rows_backward(grad_mid, mid_ref, gain_ref, gain_grad, store_grad)


def feed_forward(mid, gain, cot_full, gate_up, down_t, collective):
    count = lax.axis_size("tensor")
    rows, width = mid.shape
    hidden = down_t.shape[1]
    everything = count * rows
    return pl.pallas_call(
        functools.partial(ffn_kernel, count),
        out_shape=[
            jax.ShapeDtypeStruct((rows, width), F32),
            jax.ShapeDtypeStruct((1, width), F32),
            jax.ShapeDtypeStruct((everything, width), BF16),
            jax.ShapeDtypeStruct((width, 3 * hidden), BF16),
        ],
        in_specs=[IN_VMEM, IN_VMEM, IN_HBM, IN_HBM, IN_HBM],
        out_specs=[IN_VMEM, IN_VMEM, IN_HBM, IN_HBM],
        scratch_shapes=gather_scratch(count, rows, width)
        + scatter_scratch(count, rows, width)
        + [
            pltpu.VMEM((everything, width), BF16),
            pltpu.VMEM(gate_up.shape, BF16),
            pltpu.VMEM(down_t.shape, BF16),
            pltpu.VMEM((everything, hidden), BF16),
            pltpu.VMEM((everything, 2 * hidden), BF16),
            pltpu.VMEM((2, tile_of(width), tile_of(hidden)), BF16),
            DMA((3,)),
            DMA((2,)),
        ],
        compiler_params=params(collective),
        cost_estimate=pl.CostEstimate(
            flops=18 * everything * width * hidden,
            transcendentals=everything * hidden,
            bytes_accessed=160 * everything * width,
        ),
        name="feed_forward",
    )(mid, gain[None], cot_full, gate_up, down_t)


def residual_kernel(
    count, grad_ref, mid_ref, part_hbm, weights_hbm, attended,
    hidden_out, grad_attended, weight_grad,
    full, gather_sems, came, going, scatter_sems, total, out_t, loads, out_loads,
):
    here = lax.axis_index("tensor")
    rows, width = mid_ref.shape
    tile = tile_of(width)
    greet_line(here, count)
    out_columns = pl.ds(weights_hbm.shape[1] - out_t.shape[1], out_t.shape[1])
    get_out = pltpu.make_async_copy(weights_hbm.at[:, out_columns], out_t, out_loads.at[0])
    get_out.start()
    full[span(here, rows), :] = grad_ref[...].astype(BF16)

    def fetch(index):
        return pltpu.make_async_copy(
            part_hbm.at[span(index, rows)], going.at[index], loads.at[index]
        )

    loop(0, count, lambda index: fetch(index).start())
    gather = LineGather(here, count, rows, full, gather_sems)
    scatter = LineScatter(here, count, came, going, scatter_sems)
    meet_line(here, count)
    gather.begin()
    loop(0, count, lambda index: fetch(index).wait())
    scatter.step(0)
    total[...] = mid_ref[...] + going[here].astype(F32)

    def backward(index):
        block = span(index, rows)
        grad_attended[block, :] = matmul(full[block, :], out_t[...], NN).astype(BF16)

    get_out.wait()
    gather.each(0, backward)

    def pass_on(hop):
        gather.arrive(hop)

        @pl.when(hop < count - 1)
        def _():
            scatter.step(hop)

        gather.each(hop, backward)

    loop(1, count, pass_on)

    def column(k):
        out_t[span(k, tile), :] = matmul(full[:, span(k, tile)], attended[...], TN).astype(BF16)

    loop(0, width // tile, column)
    put_out = pltpu.make_async_copy(out_t, weight_grad.at[:, out_columns], out_loads.at[0])
    put_out.start()
    scatter.finish(total)
    gather.finish()
    hidden_out[...] = total[...].astype(BF16)
    put_out.wait()


def residual_gather(grad_mid, mid, out_part, weights, attended, collective):
    count = lax.axis_size("tensor")
    rows, width = mid.shape
    return pl.pallas_call(
        functools.partial(residual_kernel, count),
        out_shape=[
            jax.ShapeDtypeStruct((rows, width), BF16),
            jax.ShapeDtypeStruct(attended.shape, BF16),
            jax.ShapeDtypeStruct(weights.shape, BF16),
        ],
        in_specs=[IN_VMEM, IN_VMEM, IN_HBM, IN_HBM, IN_VMEM],
        out_specs=[IN_VMEM, IN_VMEM, IN_HBM],
        scratch_shapes=gather_scratch(count, rows, width)
        + scatter_scratch(count, rows, width)
        + [
            pltpu.VMEM((rows, width), F32),
            pltpu.VMEM((width, attended.shape[1]), BF16),
            DMA((count,)),
            DMA((1,)),
        ],
        compiler_params=params(collective),
        cost_estimate=pl.CostEstimate(
            flops=4 * count * rows * width * attended.shape[1],
            transcendentals=0,
            bytes_accessed=80 * count * rows * width,
        ),
        name="residual_gather",
    )(grad_mid, mid, out_part, weights, attended)


def last_kernel(
    count, grads, weights, hidden_ref, gain_ref, grad_mid, hidden_grad, gain_grad,
    came, going, scatter_sems, total,
):
    here = lax.axis_index("tensor")
    rows, width = hidden_ref.shape
    tile = tile_of(width)
    greet_line(here, count)

    def term(index, store):
        left = grads[span(index, rows), :]

        def column(k):
            store(span(k, tile), matmul(left, weights[span(k, tile), : left.shape[1]], NT))

        loop(0, width // tile, column)

    def part(index):
        def store(columns, value):
            going[index, :, columns] = value.astype(BF16)

        term(index, store)

    def own_term(columns, value):
        total[:, columns] = value

    scatter = LineScatter(here, count, came, going, scatter_sems)
    scatter.each(0, part)
    meet_line(here, count)
    scatter.step(0)
    term(here, own_term)

    def scatter_hop(hop):
        scatter.each(hop, part)
        scatter.step(hop)

    loop(1, count - 1, scatter_hop)
    scatter.finish(total)

    def store_grad(block, value):
        hidden_grad[block, :] = (grad_mid[block, :] + value).astype(BF16)

    norm_rows_backward(total, hidden_ref, gain_ref, gain_grad, store_grad)


def last_scatter(grads, weights, hidden, gain, grad_mid, collective):
    count = lax.axis_size("tensor")
    rows, width = hidden.shape
    return pl.pallas_call(
        functools.partial(last_kernel, count),
        out_shape=[
            jax.ShapeDtypeStruct((rows, width), BF16),
            jax.ShapeDtypeStruct((1, width), F32),
        ],
        in_specs=[IN_VMEM] * 5,
        out_specs=[IN_VMEM] * 2,
        scratch_shapes=scatter_scratch(count, rows, width) + [pltpu.VMEM((rows, width), F32)],
        compiler_params=params(collective),
        cost_estimate=pl.CostEstimate(
            flops=0, transcendentals=0, bytes_accessed=64 * count * rows * width
        ),
        name="last_scatter",
    )(grads, weights, hidden, gain[None], grad_mid)


def rope_of(values, cosine, signed_sine):
    return values * cosine + pltpu.roll(values, HEAD_DIM // 2, 1) * signed_sine


def rope_back(grad, cosine, signed_sine):
    return grad * cosine - pltpu.roll(grad, HEAD_DIM // 2, 1) * signed_sine


def head_columns(index):
    return pl.ds(pl.multiple_of(index * HEAD_DIM, HEAD_DIM), HEAD_DIM)


def attention_kernel(
    heads, kv_heads, sequence, normed_hbm, weights_hbm, cosine, signed_sine, query_gain, key_gain,
    raw, rotated, attended, normed, weights, loads,
):
    rows = normed.shape[0]
    width = (heads + 2 * kv_heads) * HEAD_DIM
    block = math.gcd(rows, 256)
    get_weights = pltpu.make_async_copy(weights_hbm.at[:, pl.ds(0, width)], weights, loads.at[0])
    get_normed = pltpu.make_async_copy(normed_hbm, normed, loads.at[1])
    get_weights.start()
    get_normed.start()
    get_weights.wait()
    get_normed.wait()
    positions = sequence // block

    def project(index):
        here = span(index, block)
        table = span(index % positions, block)
        cos, sin = cosine[table, :], signed_sine[table, :]
        left = normed[here, :]
        groups = 4 if (heads + kv_heads) % 4 == 0 and (2 * kv_heads) % 4 == 0 else 1
        for first in range(0, heads + 2 * kv_heads, groups):
            several = slice(first * HEAD_DIM, (first + groups) * HEAD_DIM)
            made = matmul(left, weights[:, several], NN)
            for k in range(groups):
                head = first + k
                columns = slice(head * HEAD_DIM, (head + 1) * HEAD_DIM)
                value = made[:, k * HEAD_DIM : (k + 1) * HEAD_DIM]
                if head < heads + kv_heads:
                    raw[here, columns] = value
                    gain = query_gain if head < heads else key_gain
                    inverse = lax.rsqrt(
                        jnp.mean(value * value, axis=-1, keepdims=True) + EPSILON
                    )
                    value = rope_of(value * inverse * gain[...], cos, sin)
                rotated[here, columns] = value.astype(BF16)

    loop(0, rows // block, project)
    scale = 1.0 / math.sqrt(HEAD_DIM)

    def one_head(index):
        start, head = (index // heads) * sequence, index % heads
        kv = head // (heads // kv_heads)
        for k in range(positions):
            length = (k + 1) * block
            here = pl.ds(pl.multiple_of(start + k * block, block), block)
            keys = pl.ds(pl.multiple_of(start, block), length)
            query = rotated[here, head_columns(head)]
            scores = matmul(query, rotated[keys, head_columns(heads + kv)], NT) * scale
            at_row = lax.broadcasted_iota(jnp.int32, scores.shape, 0) + k * block
            at_column = lax.broadcasted_iota(jnp.int32, scores.shape, 1)
            scores = jnp.where(at_column <= at_row, scores, NEG_FILL)
            powers = jnp.exp(scores - jnp.max(scores, axis=-1, keepdims=True))
            probs = powers * (1.0 / jnp.sum(powers, axis=-1, keepdims=True))
            attended[here, head_columns(head)] = matmul(
                probs.astype(BF16), rotated[keys, head_columns(heads + kv_heads + kv)], NN
            ).astype(BF16)

    loop(0, (rows // sequence) * heads, one_head)


def attention_forward(normed, weights, tables, gains, heads, kv_heads):
    rows, width = normed.shape
    across = (heads + 2 * kv_heads) * HEAD_DIM
    return pl.pallas_call(
        functools.partial(attention_kernel, heads, kv_heads, SEQ_LEN),
        out_shape=[
            jax.ShapeDtypeStruct((rows, (heads + kv_heads) * HEAD_DIM), F32),
            jax.ShapeDtypeStruct((rows, across), BF16),
            jax.ShapeDtypeStruct((rows, heads * HEAD_DIM), BF16),
        ],
        in_specs=[IN_HBM] * 2 + [IN_VMEM] * 4,
        out_specs=[IN_VMEM] * 3,
        scratch_shapes=[
            pltpu.VMEM((rows, width), BF16),
            pltpu.VMEM((width, across), BF16),
            DMA((2,)),
        ],
        compiler_params=params(),
        cost_estimate=pl.CostEstimate(
            flops=2 * rows * width * across,
            transcendentals=rows * SEQ_LEN * heads,
            bytes_accessed=20 * rows * width,
        ),
        name="attention_forward",
    )(normed, weights, *tables, *gains)


def attention_back_kernel(
    heads, kv_heads, sequence, normed_hbm, raw, rotated, attended, grad_attended,
    cosine, signed_sine, query_gain, key_gain, given,
    grads, weight_grad, gain_grad,
    normed, grad_rot, stage, loads, stores,
):
    rows = normed.shape[0]
    block = math.gcd(rows, 256)
    positions = sequence // block
    get_normed = pltpu.make_async_copy(normed_hbm, normed, loads.at[0])
    get_normed.start()
    scale = 1.0 / math.sqrt(HEAD_DIM)
    grad_rot[:, heads * HEAD_DIM :] = jnp.zeros_like(grad_rot[:, heads * HEAD_DIM :])

    def one_head(index):
        start, head = (index // heads) * sequence, index % heads
        kv = head // (heads // kv_heads)
        key_columns, value_columns = head_columns(heads + kv), head_columns(heads + kv_heads + kv)
        for k in range(positions):
            length = (k + 1) * block
            here = pl.ds(pl.multiple_of(start + k * block, block), block)
            keys = pl.ds(pl.multiple_of(start, block), length)
            query, key = rotated[here, head_columns(head)], rotated[keys, key_columns]
            grad = grad_attended[here, head_columns(head)]
            scores = matmul(key, query, NT) * scale
            at_key = lax.broadcasted_iota(jnp.int32, scores.shape, 0)
            at_query = lax.broadcasted_iota(jnp.int32, scores.shape, 1) + k * block
            scores = jnp.where(at_key <= at_query, scores, NEG_FILL)
            powers = jnp.exp(scores - jnp.max(scores, axis=0, keepdims=True))
            probs = powers * (1.0 / jnp.sum(powers, axis=0, keepdims=True))
            product = grad.astype(F32) * attended[here, head_columns(head)].astype(F32)
            delta = jnp.sum(jnp.transpose(product), axis=0, keepdims=True)
            grad_rot[keys, value_columns] += matmul(probs.astype(BF16), grad, NN)
            grad_probs = matmul(rotated[keys, value_columns], grad, NT)
            grad_scores = (probs * (grad_probs - delta) * scale).astype(BF16)
            grad_rot[keys, key_columns] += matmul(grad_scores, query, NN)
            grad_rot[here, head_columns(head)] = matmul(grad_scores, key, TN)

    loop(0, (rows // sequence) * heads, one_head)
    gain_grad[...] = jnp.zeros_like(gain_grad)

    def unrotate(index):
        here = span(index, block)
        table = span(index % positions, block)
        cos, sin = cosine[table, :], signed_sine[table, :]
        for head in range(heads + 2 * kv_heads):
            columns = slice(head * HEAD_DIM, (head + 1) * HEAD_DIM)
            grad = grad_rot[here, columns]
            if head < heads + kv_heads:
                which = 0 if head < heads else 1
                gain = query_gain if head < heads else key_gain
                grad = rope_back(grad, cos, sin)
                value = raw[here, columns]
                inverse = lax.rsqrt(jnp.mean(value * value, axis=-1, keepdims=True) + EPSILON)
                unit = value * inverse
                gain_grad[which : which + 1, :] += jnp.sum(grad * unit, axis=0, keepdims=True)
                grad_unit = grad * gain[...]
                mean = jnp.mean(grad_unit * unit, axis=-1, keepdims=True)
                grad = inverse * (grad_unit - unit * mean)
            grads[here, columns] = grad.astype(BF16)

    loop(0, rows // block, unrotate)
    get_normed.wait()
    tile, cols = stage.shape[1:]
    wide = grads.shape[1] // cols

    def target(index):
        return weight_grad.at[span(index // wide, tile), span(index % wide, cols)]

    def put(index):
        return pltpu.make_async_copy(stage.at[index % 2], target(index), stores.at[index % 2])

    total = normed.shape[1] // tile * wide

    def weight_tile(index):
        @pl.when(index >= 2)
        def _():
            put(index - 2).wait()

        left, right = normed[:, span(index // wide, tile)], grads[:, span(index % wide, cols)]
        stage[index % 2] = matmul(left, right, TN).astype(BF16)
        put(index).start()

    loop(0, total, weight_tile)
    for index in range(max(0, total - 2), total):
        put(index).wait()


def attention_backward(normed, raw, rotated, attended, grad_attended, tables, gains, weight_grad, heads, kv_heads):
    rows, width = normed.shape
    across = (heads + 2 * kv_heads) * HEAD_DIM
    return pl.pallas_call(
        functools.partial(attention_back_kernel, heads, kv_heads, SEQ_LEN),
        out_shape=[
            jax.ShapeDtypeStruct((rows, across), BF16),
            jax.ShapeDtypeStruct(weight_grad.shape, BF16),
            jax.ShapeDtypeStruct((2, HEAD_DIM), F32),
        ],
        in_specs=[IN_HBM] + [IN_VMEM] * 8 + [IN_HBM],
        out_specs=[IN_VMEM, IN_HBM, IN_VMEM],
        input_output_aliases={9: 1},
        scratch_shapes=[
            pltpu.VMEM((rows, width), BF16),
            pltpu.VMEM((rows, across), F32),
            pltpu.VMEM((2, tile_of(width), tile_of(across)), BF16),
            DMA((1,)),
            DMA((2,)),
        ],
        compiler_params=params(),
        cost_estimate=pl.CostEstimate(
            flops=4 * rows * width * across,
            transcendentals=rows * SEQ_LEN * heads,
            bytes_accessed=30 * rows * width,
        ),
        name="attention_backward",
    )(normed, raw, rotated, attended, grad_attended, *tables, *gains, weight_grad)


def total_kernel(line, planes, x_ref, out_ref, slots, send, recv):
    plane, here = lax.axis_index("dp"), lax.axis_index("tensor")
    me, everyone = plane * line + here, line * planes
    barrier = pltpu.get_barrier_semaphore()

    def greet(index, carry):
        @pl.when(index != me)
        def _():
            pl.semaphore_signal(
                barrier, inc=1, device_id=(index // line, index % line), device_id_type=MESH
            )

        return carry

    lax.fori_loop(0, everyone, greet, 0)
    pl.semaphore_wait(barrier, everyone - 1)

    def to(index):
        return pltpu.make_async_remote_copy(
            src_ref=x_ref,
            dst_ref=slots.at[me],
            send_sem=send.at[index],
            recv_sem=recv.at[me],
            device_id=(index // line, index % line),
            device_id_type=MESH,
        )

    def came(index):
        return pltpu.make_async_remote_copy(
            src_ref=x_ref,
            dst_ref=slots.at[index],
            send_sem=send.at[index],
            recv_sem=recv.at[index],
            device_id=(index // line, index % line),
            device_id_type=MESH,
        )

    def push(index, carry):
        @pl.when(index != me)
        def _():
            to(index).start()

        return carry

    lax.fori_loop(0, everyone, push, 0)
    slots[me] = x_ref[...]

    def settle(index, carry):
        @pl.when(index != me)
        def _():
            came(index).wait_recv()
            to(index).wait_send()

        return carry

    lax.fori_loop(0, everyone, settle, 0)

    def add(index, total):
        return total + slots[index]

    out_ref[...] = lax.fori_loop(0, everyone, add, jnp.zeros(x_ref.shape, jnp.float32))


def total_over_all(x, collective):
    line, planes = lax.axis_size("tensor"), lax.axis_size("dp")
    return pl.pallas_call(
        functools.partial(total_kernel, line, planes),
        out_shape=jax.ShapeDtypeStruct(x.shape, x.dtype),
        in_specs=[pl.BlockSpec(memory_space=pltpu.VMEM)],
        out_specs=pl.BlockSpec(memory_space=pltpu.VMEM),
        scratch_shapes=[
            pltpu.VMEM((line * planes,) + x.shape, x.dtype),
            pltpu.SemaphoreType.DMA((line * planes,)),
            pltpu.SemaphoreType.DMA((line * planes,)),
        ],
        compiler_params=pltpu.CompilerParams(collective_id=collective, has_side_effects=True),
    )(x)


def rope_tables(positions, width):
    half_width = width // 2
    freqs = ROPE_BASE ** (-(jnp.arange(half_width, dtype=F32) * (2.0 / width)))
    angles = positions.astype(F32)[:, None] * freqs[None, :]
    cosine, sine = jnp.cos(angles), jnp.sin(angles)
    return (
        jnp.concatenate([cosine, cosine], axis=1),
        jnp.concatenate([-sine, sine], axis=1),
    )


def per_device(
    hidden_in,
    query_proj,
    key_proj,
    value_proj,
    out_proj,
    gate_proj,
    up_proj,
    down_proj,
    attn_norm,
    query_norm,
    key_norm,
    ffn_norm,
    cotangent,
):
    heads_width, kv_width = query_proj.shape[1], key_proj.shape[1]
    heads, kv_heads = heads_width // HEAD_DIM, kv_width // HEAD_DIM
    qkv_width = heads_width + 2 * kv_width
    attn_full = lax.all_gather(
        jnp.concatenate([query_proj, key_proj, value_proj, out_proj.T], axis=1),
        "dp",
        axis=0,
        tiled=True,
    )
    normed = first_gather(hidden_in, attn_norm, 0)
    down_full_t = lax.all_gather(down_proj.T, "dp", axis=0, tiled=True)
    gate_up_full = lax.all_gather(
        jnp.concatenate([gate_proj, up_proj], axis=1), "dp", axis=0, tiled=True
    )
    tables = rope_tables(jnp.arange(SEQ_LEN), HEAD_DIM)
    gains = (query_norm[None], key_norm[None])
    raw, rotated, attended = attention_forward(normed, attn_full, tables, gains, heads, kv_heads)
    residual_mid, cot_full = middle_scatter(attended, attn_full, hidden_in, cotangent, 1)
    grad_mid, ffn_gain_grad, out_part, ffn_grads = feed_forward(
        residual_mid, ffn_norm, cot_full, gate_up_full, down_full_t, 2
    )

    def scatter(parts):
        return lax.psum_scatter(parts, "dp", scatter_dimension=0, tiled=True)

    ffn_sums = scatter(ffn_grads)
    hidden_out, grad_attended, attn_grads = residual_gather(
        grad_mid, residual_mid, out_part, attn_full, attended, 3
    )
    grads, attn_grads, head_gain_grads = attention_backward(
        normed, raw, rotated, attended, grad_attended, tables, gains, attn_grads, heads, kv_heads
    )
    attn_grads, ffn_sums = lax.optimization_barrier((attn_grads, ffn_sums))
    attn_sums = scatter(attn_grads)
    dhidden_in, attn_gain_grad = last_scatter(grads, attn_full, hidden_in, attn_norm, grad_mid, 4)
    parts = (attn_gain_grad, ffn_gain_grad, head_gain_grads)
    packed = jnp.concatenate([part.reshape(-1, HEAD_DIM) for part in parts])
    gain_total = total_over_all(packed, 5)
    cut = attn_norm.shape[0] // HEAD_DIM
    gate_sum, up_sum, down_sum_t = jnp.split(ffn_sums.astype(F32), 3, axis=1)
    query_sum, key_sum, value_sum, out_sum_t = jnp.split(
        attn_sums.astype(F32), [heads_width, heads_width + kv_width, qkv_width], axis=1
    )
    return (
        hidden_out,
        dhidden_in,
        query_sum,
        key_sum,
        value_sum,
        out_sum_t.T,
        gate_sum,
        up_sum,
        down_sum_t.T,
        gain_total[:cut].reshape(-1),
        gain_total[2 * cut],
        gain_total[2 * cut + 1],
        gain_total[cut : 2 * cut].reshape(-1),
    )


def solution(mesh):
    placed = (
        P(("dp", "tensor"), None),
        P("dp", "tensor"),
        P("dp", "tensor"),
        P("dp", "tensor"),
        P("tensor", "dp"),
        P("dp", "tensor"),
        P("dp", "tensor"),
        P("tensor", "dp"),
        P(),
        P(),
        P(),
        P(),
        P(("dp", "tensor"), None),
    )
    return jax.shard_map(
        per_device,
        mesh=mesh,
        in_specs=placed,
        out_specs=(
            P(("dp", "tensor"), None),
            P(("dp", "tensor"), None),
            P("dp", "tensor"),
            P("dp", "tensor"),
            P("dp", "tensor"),
            P("tensor", "dp"),
            P("dp", "tensor"),
            P("dp", "tensor"),
            P("tensor", "dp"),
            P(),
            P(),
            P(),
            P(),
        ),
        check_vma=False,
    )
```

```python
import functools
import math

import jax
import jax.numpy as jnp
from jax import lax
from jax.experimental import pallas as pl
from jax.experimental.pallas import tpu as pltpu
from jax.sharding import PartitionSpec as P


HEAD_DIM = 128
SEQ_LEN = 1024


EPSILON = 1e-06
ROPE_BASE = 1000000.0
NEG_FILL = -1e30
MESH = pl.DeviceIdType.MESH
VMEM_BYTES = 63 * 2**20
TILE = 512
F32, BF16 = jnp.float32, jnp.bfloat16
NN, NT, TN = ((1,), (0,)), ((1,), (1,)), ((0,), (0,))
IN_VMEM, IN_HBM = pl.BlockSpec(memory_space=pltpu.VMEM), pl.BlockSpec(memory_space=pl.ANY)
DMA = pltpu.SemaphoreType.DMA


def matmul(left, right, dims):
    return lax.dot_general(left, right, (dims, ((), ())), preferred_element_type=F32)


def tile_of(size):
    return TILE if size % TILE == 0 else size


def span(index, size):
    return pl.ds(pl.multiple_of(index * size, size), size)


def loop(start, stop, body):
    lax.fori_loop(start, stop, lambda index, carry: (body(index), carry)[1], 0)


def params(collective=None):
    return pltpu.CompilerParams(
        collective_id=collective, has_side_effects=True, vmem_limit_bytes=VMEM_BYTES
    )


def greet_line(here, count):
    barrier = pltpu.get_barrier_semaphore()

    @pl.when(here > 0)
    def _():
        pl.semaphore_signal(barrier, inc=1, device_id={"tensor": here - 1}, device_id_type=MESH)

    @pl.when(here < count - 1)
    def _():
        pl.semaphore_signal(barrier, inc=1, device_id={"tensor": here + 1}, device_id_type=MESH)


def meet_line(here, count):
    barrier = pltpu.get_barrier_semaphore()
    inside = jnp.logical_and(here > 0, here < count - 1)

    @pl.when(inside)
    def _():
        pl.semaphore_wait(barrier, 2)

    @pl.when(jnp.logical_not(inside))
    def _():
        pl.semaphore_wait(barrier, 1)


class LineGather:
    def __init__(self, here, count, rows, full, sems):
        self.here, self.count, self.rows, self.full, self.sems = here, count, rows, full, sems

    def copy(self, index, step, src=None):
        block = self.full.at[span(index, self.rows)]
        return pltpu.make_async_remote_copy(
            src_ref=block if src is None else src,
            dst_ref=block,
            send_sem=self.sems.at[0 if step > 0 else 1, index],
            recv_sem=self.sems.at[2, index],
            device_id={"tensor": self.here + step},
            device_id_type=MESH,
        )

    def begin(self, own=None):
        @pl.when(self.here < self.count - 1)
        def _():
            self.copy(self.here, 1, own).start()

        @pl.when(self.here > 0)
        def _():
            self.copy(self.here, -1, own).start()

    def arrive(self, hop):
        here, count = self.here, self.count

        @pl.when(here >= hop)
        def _():
            self.copy(here - hop, 1).wait_recv()

            @pl.when(here < count - 1)
            def _():
                self.copy(here - hop, 1).start()

        @pl.when(here < count - hop)
        def _():
            self.copy(here + hop, -1).wait_recv()

            @pl.when(here > 0)
            def _():
                self.copy(here + hop, -1).start()

    def each(self, hop, then):
        def side(which):
            index = self.here + (2 * which - 1) * hop
            fits = jnp.logical_and(index >= 0, index < self.count)

            @pl.when(jnp.logical_and(fits, which + hop > 0))
            def _():
                then(index)

        loop(0, 2, side)

    def pass_on(self, hop):
        here, count = self.here, self.count

        @pl.when(jnp.logical_and(here >= hop, here < count - 1))
        def _():
            self.copy(here - hop, 1).start()

        @pl.when(jnp.logical_and(here < count - hop, here > 0))
        def _():
            self.copy(here + hop, -1).start()

    def finish(self, first=0):
        here, count = self.here, self.count

        def settle(hop):
            @pl.when(jnp.logical_and(here >= hop, here < count - 1))
            def _():
                self.copy(here - hop, 1).wait_send()

            @pl.when(jnp.logical_and(here < count - hop, here > 0))
            def _():
                self.copy(here + hop, -1).wait_send()

        loop(first, count, settle)


class LineScatter:
    def __init__(self, here, count, came, going, sems):
        self.here, self.count, self.came, self.going, self.sems = here, count, came, going, sems

    def right(self, index):
        return pltpu.make_async_remote_copy(
            src_ref=self.going.at[index],
            dst_ref=self.came.at[index + 1],
            send_sem=self.sems.at[0, index],
            recv_sem=self.sems.at[1, index],
            device_id={"tensor": self.here + 1},
            device_id_type=MESH,
        )

    def left(self, index):
        return pltpu.make_async_remote_copy(
            src_ref=self.going.at[index],
            dst_ref=self.came.at[index],
            send_sem=self.sems.at[2, index],
            recv_sem=self.sems.at[3, index],
            device_id={"tensor": self.here - 1},
            device_id_type=MESH,
        )

    def goes_right(self, hop):
        return jnp.logical_and(hop >= self.here, self.here < self.count - 1)

    def goes_left(self, hop):
        return jnp.logical_and(hop >= self.count - 1 - self.here, self.here > 0)

    def rightward(self, hop):
        return self.count - 1 + self.here - hop

    def leftward(self, hop):
        return hop + self.here + 1 - self.count

    def each(self, hop, then):
        def side(which):
            goes = jnp.where(which == 0, self.goes_right(hop), self.goes_left(hop))

            @pl.when(goes)
            def _():
                then((1 - which) * self.rightward(hop) + which * self.leftward(hop))

        loop(0, 2, side)

    def add(self, index, slot):
        self.going[index] = (
            self.going[index].astype(F32) + self.came[slot].astype(F32)
        ).astype(BF16)

    def step(self, hop, send=True):
        here, count = self.here, self.count

        @pl.when(self.goes_right(hop))
        def _():
            index = self.rightward(hop)

            @pl.when(here > 0)
            def _():
                self.right(index).wait_recv()
                self.add(index, index + 1)

            if send:
                self.right(index).start()

        @pl.when(self.goes_left(hop))
        def _():
            index = self.leftward(hop)

            @pl.when(here < count - 1)
            def _():
                self.left(index).wait_recv()
                self.add(index, index)

            if send:
                self.left(index).start()

    def settle(self, hops):
        def sent(hop):
            @pl.when(self.goes_right(hop))
            def _():
                self.right(self.rightward(hop)).wait_send()

            @pl.when(self.goes_left(hop))
            def _():
                self.left(self.leftward(hop)).wait_send()

        loop(0, hops, sent)

    def finish(self, total):
        here, count = self.here, self.count

        @pl.when(here > 0)
        def _():
            self.right(here).wait_recv()
            total[...] += self.came[here + 1].astype(F32)

        @pl.when(here < count - 1)
        def _():
            self.left(here).wait_recv()
            total[...] += self.came[here].astype(F32)

        self.settle(count - 1)


class Neighbours:
    def __init__(self, here, count, to_right, to_left, lands, sems):
        self.here, self.count, self.lands, self.sems = here, count, lands, sems
        self.to_right, self.to_left = to_right, to_left

    def copy(self, side):
        return pltpu.make_async_remote_copy(
            src_ref=self.to_left if side else self.to_right,
            dst_ref=self.lands.at[side],
            send_sem=self.sems.at[0, side],
            recv_sem=self.sems.at[1, side],
            device_id={"tensor": self.here + (-1 if side else 1)},
            device_id_type=MESH,
        )

    def begin(self):
        @pl.when(self.here < self.count - 1)
        def _():
            self.copy(0).start()

        @pl.when(self.here > 0)
        def _():
            self.copy(1).start()

    def finish(self):
        @pl.when(self.here < self.count - 1)
        def _():
            self.copy(0).wait_send()
            self.copy(1).wait_recv()

        @pl.when(self.here > 0)
        def _():
            self.copy(1).wait_send()
            self.copy(0).wait_recv()


def scatter_scratch(count, rows, width):
    return [
        pltpu.VMEM((count + 1, rows, width), BF16),
        pltpu.VMEM((count, rows, width), BF16),
        DMA((4, count)),
    ]


def gather_scratch(count, rows, width):
    return [pltpu.VMEM((count * rows, width), BF16), DMA((3, count))]


def row_blocks(rows):
    return 64 if rows % 64 == 0 else rows


def norm_rows(values_ref, gain_ref, store):
    block = row_blocks(values_ref.shape[0])

    def body(index):
        rows = span(index, block)
        values = values_ref[rows, :].astype(F32)
        inverse = lax.rsqrt(jnp.mean(values * values, axis=-1, keepdims=True) + EPSILON)
        store(rows, values * inverse * gain_ref[...])

    loop(0, values_ref.shape[0] // block, body)


def norm_rows_backward(grad_ref, values_ref, gain_ref, gain_grad_ref, store):
    block = row_blocks(values_ref.shape[0])
    gain_grad_ref[...] = jnp.zeros_like(gain_grad_ref)

    def body(index):
        rows = span(index, block)
        values, grad = values_ref[rows, :].astype(F32), grad_ref[rows, :]
        inverse = lax.rsqrt(jnp.mean(values * values, axis=-1, keepdims=True) + EPSILON)
        unit = values * inverse
        grad_unit = grad * gain_ref[...]
        mean = jnp.mean(grad_unit * unit, axis=-1, keepdims=True)
        gain_grad_ref[...] += jnp.sum(grad * unit, axis=0, keepdims=True)
        store(rows, inverse * (grad_unit - unit * mean))

    loop(0, values_ref.shape[0] // block, body)


def first_kernel(
    count, hidden_ref, gain_ref, up_ref, down_ref, out_ref, late_ref, full, sems, done
):
    here = lax.axis_index("tensor")
    rows = hidden_ref.shape[0]
    greet_line(here, count)
    own = full.at[span(here, rows)]

    def store(block, normed):
        own[block, :] = normed.astype(BF16)

    norm_rows(hidden_ref, gain_ref, store)
    meet_line(here, count)
    line = LineGather(here, count, rows, full, sems)
    line.begin()
    late_ref[:, : up_ref.shape[1]] = up_ref[...]
    tile = tile_of(down_ref.shape[0])

    def turn(index):
        columns = pl.ds(pl.multiple_of(up_ref.shape[1] + index * tile, tile), tile)
        late_ref[:, columns] = jnp.transpose(down_ref[span(index, tile), :])

    loop(0, down_ref.shape[0] // tile, turn)

    def put(index):
        return pltpu.make_async_copy(
            full.at[span(index, rows)], out_ref.at[span(index, rows)], done.at[index]
        )

    def pass_on(hop):
        @pl.when(hop > 0)
        def _():
            line.arrive(hop)

        line.each(hop, lambda index: put(index).start())

    loop(0, count, pass_on)
    loop(0, count, lambda index: put(index).wait())
    line.finish()


def first_gather(hidden, gain, up, down, collective):
    count = lax.axis_size("tensor")
    rows, width = hidden.shape
    return pl.pallas_call(
        functools.partial(first_kernel, count),
        out_shape=[
            jax.ShapeDtypeStruct((count * rows, width), BF16),
            jax.ShapeDtypeStruct((up.shape[0], up.shape[1] + down.shape[0]), BF16),
        ],
        in_specs=[IN_VMEM] * 4,
        out_specs=[IN_HBM, IN_VMEM],
        scratch_shapes=gather_scratch(count, rows, width) + [DMA((count,))],
        compiler_params=params(collective),
        cost_estimate=pl.CostEstimate(
            flops=0, transcendentals=0, bytes_accessed=64 * count * rows * width
        ),
        name="first_gather",
    )(hidden, gain[None], up, down)


def middle_kernel(
    count, attended, weights, hidden_ref, cot_ref, near, mid_ref, cot_out,
    came, going, scatter_sems, full, gather_sems, done, near_done,
):
    here = lax.axis_index("tensor")
    rows, width = hidden_ref.shape
    tile = tile_of(width)
    out_columns = slice(weights.shape[1] - attended.shape[1], weights.shape[1])
    greet_line(here, count)

    def term(index, store):
        left = attended[span(index, rows), :]

        def column(k):
            store(span(k, tile), matmul(left, weights[span(k, tile), out_columns], NT))

        loop(0, width // tile, column)

    def part(index):
        def store(columns, value):
            going[index, :, columns] = value.astype(BF16)

        term(index, store)

    scatter = LineScatter(here, count, came, going, scatter_sems)
    gather = LineGather(here, count, rows, full, gather_sems)

    def put(index):
        return pltpu.make_async_copy(
            full.at[span(index, rows)], cot_out.at[span(index, rows)], done.at[index]
        )

    own = pltpu.make_async_copy(cot_ref, cot_out.at[span(here, rows)], done.at[here])
    own.start()

    def fetch(side):
        return pltpu.make_async_copy(
            near.at[side], full.at[span(here + 2 * side - 1, rows)], near_done.at[side]
        )

    def beside(then):
        @pl.when(here > 0)
        def _():
            then(0)

        @pl.when(here < count - 1)
        def _():
            then(1)

    beside(lambda side: fetch(side).start())
    scatter.each(0, part)
    meet_line(here, count)
    scatter.step(0)
    beside(lambda side: fetch(side).wait())
    gather.pass_on(1)
    gather.each(1, lambda index: put(index).start())

    def own_term(columns, value):
        mid_ref[:, columns] = hidden_ref[:, columns].astype(F32) + value

    term(here, own_term)

    def pass_on(hop):
        scatter.each(hop, part)
        scatter.step(hop)
        gather.arrive(hop + 1)
        gather.each(hop + 1, lambda index: put(index).start())

    loop(1, count - 1, pass_on)
    scatter.finish(mid_ref)
    own.wait()

    def settle(index):
        @pl.when(index != here)
        def _():
            put(index).wait()

    loop(0, count, settle)
    gather.finish(1)


def middle_scatter(attended, weights, hidden, cotangent, near, collective):
    count = lax.axis_size("tensor")
    rows, width = hidden.shape
    return pl.pallas_call(
        functools.partial(middle_kernel, count),
        out_shape=[
            jax.ShapeDtypeStruct((rows, width), F32),
            jax.ShapeDtypeStruct((count * rows, width), BF16),
        ],
        in_specs=[IN_VMEM] * 4 + [IN_HBM],
        out_specs=[IN_VMEM, IN_HBM],
        scratch_shapes=scatter_scratch(count, rows, width)
        + gather_scratch(count, rows, width)
        + [DMA((count,)), DMA((2,))],
        compiler_params=params(collective),
        cost_estimate=pl.CostEstimate(
            flops=0, transcendentals=0, bytes_accessed=80 * count * rows * width
        ),
        name="middle_scatter",
    )(attended, weights, hidden, cotangent, near)


def ffn_kernel(
    count, mid_ref, gain_ref, cot_hbm, gate_hbm, late_hbm,
    grad_mid, gain_grad, out_part, weight_grad,
    full, gather_sems, came, going, scatter_sems,
    cot, gate_up, down_t, act, grads, stage, loads, stores,
):
    here = lax.axis_index("tensor")
    rows, width = mid_ref.shape
    hidden = down_t.shape[1]
    cols, tile = tile_of(hidden), tile_of(width)
    greet_line(here, count)
    low, high = pl.ds(0, hidden), pl.ds(hidden, hidden)
    fetches = [
        pltpu.make_async_copy(src, dst, loads.at[k])
        for k, (src, dst) in enumerate(
            (
                (cot_hbm, cot),
                (late_hbm.at[:, high], down_t),
                (gate_hbm, gate_up.at[:, low]),
                (late_hbm.at[:, low], gate_up.at[:, high]),
            )
        )
    ]
    for fetch in fetches:
        fetch.start()
    own = full.at[span(here, rows)]

    def store_normed(block, normed):
        own[block, :] = normed.astype(BF16)

    norm_rows(mid_ref, gain_ref, store_normed)
    meet_line(here, count)
    gather = LineGather(here, count, rows, full, gather_sems)
    scatter = LineScatter(here, count, came, going, scatter_sems)
    gather.begin()
    fetches[0].wait()
    fetches[1].wait()

    def grad_hidden(index):
        block, columns = span(index // (hidden // cols), rows), span(index % (hidden // cols), cols)
        grads[block, columns] = matmul(cot[block, :], down_t[:, columns], NN).astype(BF16)

    loop(0, count * (hidden // cols), grad_hidden)
    fetches[2].wait()
    fetches[3].wait()

    def forward(index):
        block = span(index, rows)

        def column(k):
            here_cols, up_cols = span(k, cols), pl.ds(pl.multiple_of(hidden + k * cols, cols), cols)
            gate = matmul(full[block, :], gate_up[:, here_cols], NN)
            up = matmul(full[block, :], gate_up[:, up_cols], NN)
            grad = grads[block, here_cols].astype(F32)
            sigmoid = jax.nn.sigmoid(gate)
            silu = gate * sigmoid
            act[block, here_cols] = (silu * up).astype(BF16)
            grads[block, up_cols] = (grad * silu).astype(BF16)
            grads[block, here_cols] = (
                grad * up * sigmoid * (1.0 + gate * (1.0 - sigmoid))
            ).astype(BF16)

        loop(0, hidden // cols, column)

    def pass_on(hop):
        @pl.when(hop > 0)
        def _():
            gather.arrive(hop)

        gather.each(hop, forward)

    loop(0, count, pass_on)

    def term(index, store):
        block = span(index, rows)

        def column(k):
            store(span(k, tile), matmul(grads[block, :], gate_up[span(k, tile), :], NT))

        loop(0, width // tile, column)

    def part(index):
        def store(columns, value):
            going[index, :, columns] = value.astype(BF16)

        term(index, store)

    def own_term(columns, value):
        grad_mid[:, columns] = value

    def put(slot, target):
        return pltpu.make_async_copy(stage.at[slot], target, stores.at[slot])

    def stream(total, compute, target):
        def body(index):
            slot = index % 2

            @pl.when(index >= 2)
            def _():
                put(slot, target(index - 2)).wait()

            stage[slot] = compute(index).astype(BF16)
            put(slot, target(index)).start()

        loop(0, total, body)
        for index in range(max(0, total - 2), total):
            put(index % 2, target(index)).wait()

    across = width // tile

    def output_tile(index):
        return matmul(
            act[span(index // across, tile), :], down_t[span(index % across, tile), :], NT
        )

    def output_target(index):
        return out_part.at[span(index // across, tile), span(index % across, tile)]

    wide = hidden // cols

    def down_tile(index):
        return matmul(cot[:, span(index // wide, tile)], act[:, span(index % wide, cols)], TN)

    def down_target(index):
        columns = pl.ds(pl.multiple_of((2 * wide + index % wide) * cols, cols), cols)
        return weight_grad.at[span(index // wide, tile), columns]

    def gate_up_tile(index):
        return matmul(
            full[:, span(index // (2 * wide), tile)], grads[:, span(index % (2 * wide), cols)], TN
        )

    def gate_up_target(index):
        return weight_grad.at[span(index // (2 * wide), tile), span(index % (2 * wide), cols)]

    def scatter_hop(hop):
        scatter.each(hop, part)
        scatter.step(hop)

        @pl.when(hop == 0)
        def _():
            term(here, own_term)
            stream(count * rows // tile * across, output_tile, output_target)

        @pl.when(hop == 1)
        def _():
            stream(across * wide, down_tile, down_target)

    loop(0, count - 1, scatter_hop)
    stream(across * 2 * wide, gate_up_tile, gate_up_target)
    scatter.finish(grad_mid)
    gather.finish()

    def store_grad(block, value):
        rows_here = pl.ds(here * rows + block.start, block.size)
        grad_mid[block, :] = cot[rows_here, :].astype(F32) + value

    norm_rows_backward(grad_mid, mid_ref, gain_ref, gain_grad, store_grad)


def feed_forward(mid, gain, cot_full, gate, late, collective):
    count = lax.axis_size("tensor")
    rows, width = mid.shape
    hidden = gate.shape[1]
    everything = count * rows
    return pl.pallas_call(
        functools.partial(ffn_kernel, count),
        out_shape=[
            jax.ShapeDtypeStruct((rows, width), F32),
            jax.ShapeDtypeStruct((1, width), F32),
            jax.ShapeDtypeStruct((everything, width), BF16),
            jax.ShapeDtypeStruct((width, 3 * hidden), BF16),
        ],
        in_specs=[IN_VMEM, IN_VMEM, IN_HBM, IN_HBM, IN_HBM],
        out_specs=[IN_VMEM, IN_VMEM, IN_HBM, IN_HBM],
        scratch_shapes=gather_scratch(count, rows, width)
        + scatter_scratch(count, rows, width)
        + [
            pltpu.VMEM((everything, width), BF16),
            pltpu.VMEM((width, 2 * hidden), BF16),
            pltpu.VMEM((width, hidden), BF16),
            pltpu.VMEM((everything, hidden), BF16),
            pltpu.VMEM((everything, 2 * hidden), BF16),
            pltpu.VMEM((2, tile_of(width), tile_of(hidden)), BF16),
            DMA((4,)),
            DMA((2,)),
        ],
        compiler_params=params(collective),
        cost_estimate=pl.CostEstimate(
            flops=18 * everything * width * hidden,
            transcendentals=everything * hidden,
            bytes_accessed=160 * everything * width,
        ),
        name="feed_forward",
    )(mid, gain[None], cot_full, gate, late)


def residual_kernel(
    count, grad_ref, mid_ref, part_hbm, weights_hbm, attended,
    total, near, grad_attended, weight_grad,
    full, gather_sems, came, going, scatter_sems, out_t, loads, out_loads, near_sems,
):
    here = lax.axis_index("tensor")
    rows, width = mid_ref.shape
    tile = tile_of(width)
    greet_line(here, count)
    out_columns = pl.ds(weights_hbm.shape[1] - out_t.shape[1], out_t.shape[1])
    get_out = pltpu.make_async_copy(weights_hbm.at[:, out_columns], out_t, out_loads.at[0])
    get_out.start()
    full[span(here, rows), :] = grad_ref[...].astype(BF16)

    def fetch(index):
        return pltpu.make_async_copy(
            part_hbm.at[span(index, rows)], going.at[index], loads.at[index]
        )

    loop(0, count, lambda index: fetch(index).start())
    gather = LineGather(here, count, rows, full, gather_sems)
    scatter = LineScatter(here, count, came, going, scatter_sems)
    meet_line(here, count)
    gather.begin()
    loop(0, count, lambda index: fetch(index).wait())

    def scatter_hop(hop):
        @pl.when(hop < count - 2)
        def _():
            scatter.step(hop)

    scatter_hop(0)
    total[...] = mid_ref[...] + going[here].astype(F32)

    def backward(index):
        block = span(index, rows)
        grad_attended[block, :] = matmul(full[block, :], out_t[...], NN).astype(BF16)

    get_out.wait()
    gather.each(0, backward)

    def pass_on(hop):
        gather.arrive(hop)
        scatter_hop(hop)
        gather.each(hop, backward)

    loop(1, count, pass_on)

    def column(k):
        out_t[span(k, tile), :] = matmul(full[:, span(k, tile)], attended[...], TN).astype(BF16)

    loop(0, width // tile, column)
    put_out = pltpu.make_async_copy(out_t, weight_grad.at[:, out_columns], out_loads.at[0])
    put_out.start()
    scatter.step(count - 2, send=False)

    def hand_on(side):
        return pltpu.make_async_copy(
            going.at[here + 2 * side - 1], near.at[side], near_sems.at[side]
        )

    @pl.when(here > 0)
    def _():
        hand_on(0).start()
        hand_on(0).wait()

    @pl.when(here < count - 1)
    def _():
        hand_on(1).start()
        hand_on(1).wait()

    scatter.settle(count - 2)
    gather.finish()
    put_out.wait()


def residual_gather(grad_mid, mid, out_part, weights, attended, collective):
    count = lax.axis_size("tensor")
    rows, width = mid.shape
    return pl.pallas_call(
        functools.partial(residual_kernel, count),
        out_shape=[
            jax.ShapeDtypeStruct((rows, width), F32),
            jax.ShapeDtypeStruct((2, rows, width), BF16),
            jax.ShapeDtypeStruct(attended.shape, BF16),
            jax.ShapeDtypeStruct(weights.shape, BF16),
        ],
        in_specs=[IN_VMEM, IN_VMEM, IN_HBM, IN_HBM, IN_VMEM],
        out_specs=[IN_VMEM, IN_HBM, IN_VMEM, IN_HBM],
        scratch_shapes=gather_scratch(count, rows, width)
        + scatter_scratch(count, rows, width)
        + [
            pltpu.VMEM((width, attended.shape[1]), BF16),
            DMA((count,)),
            DMA((1,)),
            DMA((2,)),
        ],
        compiler_params=params(collective),
        cost_estimate=pl.CostEstimate(
            flops=4 * count * rows * width * attended.shape[1],
            transcendentals=0,
            bytes_accessed=80 * count * rows * width,
        ),
        name="residual_gather",
    )(grad_mid, mid, out_part, weights, attended)


def last_kernel(
    count, planes, grads, weights, hidden_ref, gain_ref, grad_mid, ready_ref, hidden_grad, sums_ref,
    came, going, scatter_sems, total, gain_grad, gains, line_sum, line_slots, slots, line_sems, sems,
):
    here = lax.axis_index("tensor")
    plane = lax.axis_index("dp")
    barrier = pltpu.get_barrier_semaphore()

    def others(total, me, then):
        def body(index):
            @pl.when(index != me)
            def _():
                then(index)

        loop(0, total, body)

    def greet(axis):
        def signal(index):
            pl.semaphore_signal(barrier, inc=1, device_id={axis: index}, device_id_type=MESH)

        return signal

    others(count, here, greet("tensor"))
    others(planes, plane, greet("dp"))

    def add_up(axis, total, me, source, slots, sems):
        def give(index, slot):
            return pltpu.make_async_remote_copy(
                src_ref=source,
                dst_ref=slots.at[slot],
                send_sem=sems.at[0, index],
                recv_sem=sems.at[1, slot],
                device_id={axis: index},
                device_id_type=MESH,
            )

        others(total, me, lambda index: give(index, me).start())
        slots[me] = source[...]

        def settle(index):
            give(index, index).wait_recv()
            give(index, me).wait_send()

        others(total, me, settle)
        return lax.fori_loop(1, total, lambda index, so_far: so_far + slots[index], slots[0])

    rows, width = hidden_ref.shape
    tile = tile_of(width)

    def term(index, store):
        left = grads[span(index, rows), :]

        def column(k):
            store(span(k, tile), matmul(left, weights[span(k, tile), : left.shape[1]], NT))

        loop(0, width // tile, column)

    def part(index):
        def store(columns, value):
            going[index, :, columns] = value.astype(BF16)

        term(index, store)

    def own_term(columns, value):
        total[:, columns] = value

    scatter = LineScatter(here, count, came, going, scatter_sems)
    scatter.each(0, part)
    pl.semaphore_wait(barrier, count + planes - 2)
    scatter.step(0)
    late = width // HEAD_DIM
    gains[late:, :] = ready_ref[...]
    term(here, own_term)

    def scatter_hop(hop):
        scatter.each(hop, part)
        scatter.step(hop)

    loop(1, count - 1, scatter_hop)
    scatter.finish(total)

    def store_grad(block, value):
        hidden_grad[block, :] = (grad_mid[block, :] + value).astype(BF16)

    norm_rows_backward(total, hidden_ref, gain_ref, gain_grad, store_grad)
    for k in range(late):
        gains[k : k + 1, :] = gain_grad[:, k * HEAD_DIM : (k + 1) * HEAD_DIM]
    line_sum[...] = add_up("tensor", count, here, gains, line_slots, line_sems)
    sums_ref[...] = add_up("dp", planes, plane, line_sum, slots, sems)


def last_scatter(grads, weights, hidden, gain, grad_mid, ready, collective):
    count, planes = lax.axis_size("tensor"), lax.axis_size("dp")
    gains = (gain.shape[0] // HEAD_DIM + ready.shape[0], HEAD_DIM)
    rows, width = hidden.shape
    return pl.pallas_call(
        functools.partial(last_kernel, count, planes),
        out_shape=[
            jax.ShapeDtypeStruct((rows, width), BF16),
            jax.ShapeDtypeStruct(gains, F32),
        ],
        in_specs=[IN_VMEM] * 6,
        out_specs=[IN_VMEM] * 2,
        scratch_shapes=scatter_scratch(count, rows, width)
        + [
            pltpu.VMEM((rows, width), F32),
            pltpu.VMEM((1, width), F32),
            pltpu.VMEM(gains, F32),
            pltpu.VMEM(gains, F32),
            pltpu.VMEM((count,) + gains, F32),
            pltpu.VMEM((planes,) + gains, F32),
            DMA((2, count)),
            DMA((2, planes)),
        ],
        compiler_params=params(collective),
        cost_estimate=pl.CostEstimate(
            flops=0, transcendentals=0, bytes_accessed=64 * count * rows * width
        ),
        name="last_scatter",
    )(grads, weights, hidden, gain[None], grad_mid, ready)


def rope_of(values, cosine, signed_sine):
    return values * cosine + pltpu.roll(values, HEAD_DIM // 2, 1) * signed_sine


def rope_back(grad, cosine, signed_sine):
    return grad * cosine - pltpu.roll(grad, HEAD_DIM // 2, 1) * signed_sine


def head_columns(index):
    return pl.ds(pl.multiple_of(index * HEAD_DIM, HEAD_DIM), HEAD_DIM)


def attention_kernel(
    count, heads, kv_heads, sequence, normed_hbm, weights_hbm, cosine, signed_sine, query_gain, key_gain, cot_hbm,
    raw, rotated, attended, near, normed, weights, loads, sems,
):
    here_on_line = lax.axis_index("tensor")
    greet_line(here_on_line, count)
    rows = normed.shape[0]
    width = (heads + 2 * kv_heads) * HEAD_DIM
    block = math.gcd(rows, 256)
    get_weights = pltpu.make_async_copy(weights_hbm.at[:, pl.ds(0, width)], weights, loads.at[0])
    get_normed = pltpu.make_async_copy(normed_hbm, normed, loads.at[1])
    get_weights.start()
    get_normed.start()
    meet_line(here_on_line, count)
    hop = Neighbours(here_on_line, count, cot_hbm, cot_hbm, near, sems)
    hop.begin()
    get_weights.wait()
    get_normed.wait()
    positions = sequence // block

    def project(index):
        here = span(index, block)
        table = span(index % positions, block)
        cos, sin = cosine[table, :], signed_sine[table, :]
        left = normed[here, :]
        groups = 4 if (heads + kv_heads) % 4 == 0 and (2 * kv_heads) % 4 == 0 else 1
        for first in range(0, heads + 2 * kv_heads, groups):
            several = slice(first * HEAD_DIM, (first + groups) * HEAD_DIM)
            made = matmul(left, weights[:, several], NN)
            for k in range(groups):
                head = first + k
                columns = slice(head * HEAD_DIM, (head + 1) * HEAD_DIM)
                value = made[:, k * HEAD_DIM : (k + 1) * HEAD_DIM]
                if head < heads + kv_heads:
                    raw[here, columns] = value
                    gain = query_gain if head < heads else key_gain
                    inverse = lax.rsqrt(
                        jnp.mean(value * value, axis=-1, keepdims=True) + EPSILON
                    )
                    value = rope_of(value * inverse * gain[...], cos, sin)
                rotated[here, columns] = value.astype(BF16)

    loop(0, rows // block, project)
    scale = 1.0 / math.sqrt(HEAD_DIM)

    def one_head(index):
        start, head = (index // heads) * sequence, index % heads
        kv = head // (heads // kv_heads)
        for k in range(positions):
            length = (k + 1) * block
            here = pl.ds(pl.multiple_of(start + k * block, block), block)
            keys = pl.ds(pl.multiple_of(start, block), length)
            query = rotated[here, head_columns(head)]
            scores = matmul(query, rotated[keys, head_columns(heads + kv)], NT) * scale
            at_row = lax.broadcasted_iota(jnp.int32, scores.shape, 0) + k * block
            at_column = lax.broadcasted_iota(jnp.int32, scores.shape, 1)
            scores = jnp.where(at_column <= at_row, scores, NEG_FILL)
            powers = jnp.exp(scores - jnp.max(scores, axis=-1, keepdims=True))
            probs = powers * (1.0 / jnp.sum(powers, axis=-1, keepdims=True))
            attended[here, head_columns(head)] = matmul(
                probs.astype(BF16), rotated[keys, head_columns(heads + kv_heads + kv)], NN
            ).astype(BF16)

    loop(0, (rows // sequence) * heads, one_head)
    hop.finish()


def attention_forward(normed, weights, tables, gains, cotangent, heads, kv_heads, collective):
    count = lax.axis_size("tensor")
    rows, width = normed.shape
    across = (heads + 2 * kv_heads) * HEAD_DIM
    return pl.pallas_call(
        functools.partial(attention_kernel, count, heads, kv_heads, SEQ_LEN),
        out_shape=[
            jax.ShapeDtypeStruct((rows, (heads + kv_heads) * HEAD_DIM), F32),
            jax.ShapeDtypeStruct((rows, across), BF16),
            jax.ShapeDtypeStruct((rows, heads * HEAD_DIM), BF16),
            jax.ShapeDtypeStruct((2,) + cotangent.shape, BF16),
        ],
        in_specs=[IN_HBM] * 2 + [IN_VMEM] * 4 + [IN_HBM],
        out_specs=[IN_VMEM] * 3 + [IN_HBM],
        scratch_shapes=[
            pltpu.VMEM((rows, width), BF16),
            pltpu.VMEM((width, across), BF16),
            DMA((2,)),
            DMA((2, 2)),
        ],
        compiler_params=params(collective),
        cost_estimate=pl.CostEstimate(
            flops=2 * rows * width * across,
            transcendentals=rows * SEQ_LEN * heads,
            bytes_accessed=20 * rows * width,
        ),
        name="attention_forward",
    )(normed, weights, *tables, *gains, cotangent)


def attention_back_kernel(
    count, heads, kv_heads, sequence, normed_hbm, raw, rotated, attended, grad_attended,
    cosine, signed_sine, query_gain, key_gain, total, near, given,
    grads, weight_grad, gain_grad, hidden_out,
    normed, grad_rot, stage, came, loads, stores, sems,
):
    here_on_line = lax.axis_index("tensor")
    greet_line(here_on_line, count)
    rows = normed.shape[0]
    block = math.gcd(rows, 256)
    positions = sequence // block
    get_normed = pltpu.make_async_copy(normed_hbm, normed, loads.at[0])
    get_normed.start()
    scale = 1.0 / math.sqrt(HEAD_DIM)
    grad_rot[:, heads * HEAD_DIM :] = jnp.zeros_like(grad_rot[:, heads * HEAD_DIM :])
    meet_line(here_on_line, count)
    hop = Neighbours(here_on_line, count, near.at[1], near.at[0], came, sems)
    hop.begin()

    def one_head(index):
        start, head = (index // heads) * sequence, index % heads
        kv = head // (heads // kv_heads)
        key_columns, value_columns = head_columns(heads + kv), head_columns(heads + kv_heads + kv)
        for k in range(positions):
            length = (k + 1) * block
            here = pl.ds(pl.multiple_of(start + k * block, block), block)
            keys = pl.ds(pl.multiple_of(start, block), length)
            query, key = rotated[here, head_columns(head)], rotated[keys, key_columns]
            grad = grad_attended[here, head_columns(head)]
            scores = matmul(key, query, NT) * scale
            at_key = lax.broadcasted_iota(jnp.int32, scores.shape, 0)
            at_query = lax.broadcasted_iota(jnp.int32, scores.shape, 1) + k * block
            scores = jnp.where(at_key <= at_query, scores, NEG_FILL)
            powers = jnp.exp(scores - jnp.max(scores, axis=0, keepdims=True))
            probs = powers * (1.0 / jnp.sum(powers, axis=0, keepdims=True))
            product = grad.astype(F32) * attended[here, head_columns(head)].astype(F32)
            delta = jnp.sum(jnp.transpose(product), axis=0, keepdims=True)
            grad_rot[keys, value_columns] += matmul(probs.astype(BF16), grad, NN)
            grad_probs = matmul(rotated[keys, value_columns], grad, NT)
            grad_scores = (probs * (grad_probs - delta) * scale).astype(BF16)
            grad_rot[keys, key_columns] += matmul(grad_scores, query, NN)
            grad_rot[here, head_columns(head)] = matmul(grad_scores, key, TN)

    loop(0, (rows // sequence) * heads, one_head)
    gain_grad[...] = jnp.zeros_like(gain_grad)

    def unrotate(index):
        here = span(index, block)
        table = span(index % positions, block)
        cos, sin = cosine[table, :], signed_sine[table, :]
        for head in range(heads + 2 * kv_heads):
            columns = slice(head * HEAD_DIM, (head + 1) * HEAD_DIM)
            grad = grad_rot[here, columns]
            if head < heads + kv_heads:
                which = 0 if head < heads else 1
                gain = query_gain if head < heads else key_gain
                grad = rope_back(grad, cos, sin)
                value = raw[here, columns]
                inverse = lax.rsqrt(jnp.mean(value * value, axis=-1, keepdims=True) + EPSILON)
                unit = value * inverse
                gain_grad[which : which + 1, :] += jnp.sum(grad * unit, axis=0, keepdims=True)
                grad_unit = grad * gain[...]
                mean = jnp.mean(grad_unit * unit, axis=-1, keepdims=True)
                grad = inverse * (grad_unit - unit * mean)
            grads[here, columns] = grad.astype(BF16)

    loop(0, rows // block, unrotate)
    get_normed.wait()
    tile, cols = stage.shape[1:]
    wide = grads.shape[1] // cols

    def target(index):
        return weight_grad.at[span(index // wide, tile), span(index % wide, cols)]

    def put(index):
        return pltpu.make_async_copy(stage.at[index % 2], target(index), stores.at[index % 2])

    tiles = normed.shape[1] // tile * wide

    def weight_tile(index):
        @pl.when(index >= 2)
        def _():
            put(index - 2).wait()

        left, right = normed[:, span(index // wide, tile)], grads[:, span(index % wide, cols)]
        stage[index % 2] = matmul(left, right, TN).astype(BF16)
        put(index).start()

    loop(0, tiles, weight_tile)
    for index in range(max(0, tiles - 2), tiles):
        put(index).wait()

    hop.finish()

    @pl.when(here_on_line == 0)
    def _():
        hidden_out[...] = (total[...] + came[1].astype(F32)).astype(BF16)

    @pl.when(here_on_line == count - 1)
    def _():
        hidden_out[...] = (total[...] + came[0].astype(F32)).astype(BF16)

    @pl.when(jnp.logical_and(here_on_line > 0, here_on_line < count - 1))
    def _():
        hidden_out[...] = (total[...] + came[0].astype(F32) + came[1].astype(F32)).astype(BF16)


def attention_backward(normed, raw, rotated, attended, grad_attended, tables, gains, total, near, weight_grad, heads, kv_heads, collective):
    count = lax.axis_size("tensor")
    rows, width = normed.shape
    across = (heads + 2 * kv_heads) * HEAD_DIM
    return pl.pallas_call(
        functools.partial(attention_back_kernel, count, heads, kv_heads, SEQ_LEN),
        out_shape=[
            jax.ShapeDtypeStruct((rows, across), BF16),
            jax.ShapeDtypeStruct(weight_grad.shape, BF16),
            jax.ShapeDtypeStruct((2, HEAD_DIM), F32),
            jax.ShapeDtypeStruct(total.shape, BF16),
        ],
        in_specs=[IN_HBM] + [IN_VMEM] * 9 + [IN_HBM] * 2,
        out_specs=[IN_VMEM, IN_HBM, IN_VMEM, IN_VMEM],
        input_output_aliases={11: 1},
        scratch_shapes=[
            pltpu.VMEM((rows, width), BF16),
            pltpu.VMEM((rows, across), F32),
            pltpu.VMEM((2, tile_of(width), tile_of(across)), BF16),
            pltpu.VMEM(near.shape, BF16),
            DMA((1,)),
            DMA((2,)),
            DMA((2, 2)),
        ],
        compiler_params=params(collective),
        cost_estimate=pl.CostEstimate(
            flops=4 * rows * width * across,
            transcendentals=rows * SEQ_LEN * heads,
            bytes_accessed=30 * rows * width,
        ),
        name="attention_backward",
    )(normed, raw, rotated, attended, grad_attended, *tables, *gains, total, near, weight_grad)


def deliver_kernel(ffn_sums, attn_sums, gains, *outs):
    query, key, value, out, gate, up, down, attn_gain, query_gain, key_gain, ffn_gain = outs

    def turned(source, first, target):
        side = tile_of(target.shape[0])
        for k in range(target.shape[0] // side):
            columns = slice(first + k * side, first + (k + 1) * side)
            target[k * side : (k + 1) * side, :] = jnp.transpose(source[:, columns].astype(F32))

    start = 0
    for target in (query, key, value):
        target[...] = attn_sums[:, start : start + target.shape[1]].astype(F32)
        start += target.shape[1]
    turned(attn_sums, start, out)
    width = gate.shape[1]
    gate[...] = ffn_sums[:, :width].astype(F32)
    up[...] = ffn_sums[:, width : 2 * width].astype(F32)
    turned(ffn_sums, 2 * width, down)
    cut = attn_gain.shape[0]
    attn_gain[...] = gains[:cut, :]
    ffn_gain[...] = gains[cut : 2 * cut, :]
    query_gain[...] = gains[2 * cut : 2 * cut + 1, :]
    key_gain[...] = gains[2 * cut + 1 : 2 * cut + 2, :]


def deliver(ffn_sums, attn_sums, gains, shapes, cut):
    shapes = list(shapes) + [(cut, HEAD_DIM), (1, HEAD_DIM), (1, HEAD_DIM), (cut, HEAD_DIM)]
    return pl.pallas_call(
        deliver_kernel,
        out_shape=[jax.ShapeDtypeStruct(shape, F32) for shape in shapes],
        in_specs=[IN_VMEM] * 3,
        out_specs=[IN_VMEM] * len(shapes),
        compiler_params=pltpu.CompilerParams(vmem_limit_bytes=VMEM_BYTES),
        name="deliver",
    )(ffn_sums, attn_sums, gains)


def rope_tables(positions, width):
    half_width = width // 2
    freqs = ROPE_BASE ** (-(jnp.arange(half_width, dtype=F32) * (2.0 / width)))
    angles = positions.astype(F32)[:, None] * freqs[None, :]
    cosine, sine = jnp.cos(angles), jnp.sin(angles)
    return (
        jnp.concatenate([cosine, cosine], axis=1),
        jnp.concatenate([-sine, sine], axis=1),
    )


def per_device(
    hidden_in,
    query_proj,
    key_proj,
    value_proj,
    out_proj,
    gate_proj,
    up_proj,
    down_proj,
    attn_norm,
    query_norm,
    key_norm,
    ffn_norm,
    cotangent,
):
    heads_width, kv_width = query_proj.shape[1], key_proj.shape[1]
    heads, kv_heads = heads_width // HEAD_DIM, kv_width // HEAD_DIM
    attn_full = lax.all_gather(
        jnp.concatenate([query_proj, key_proj, value_proj, out_proj.T], axis=1),
        "dp",
        axis=0,
        tiled=True,
    )
    gate_full = lax.all_gather(gate_proj, "dp", axis=0, tiled=True)
    normed, late = first_gather(hidden_in, attn_norm, up_proj, down_proj, 0)
    late_full = lax.all_gather(late, "dp", axis=0, tiled=True)
    tables = rope_tables(jnp.arange(SEQ_LEN), HEAD_DIM)
    gains = (query_norm[None], key_norm[None])
    raw, rotated, attended, cot_near = attention_forward(
        normed, attn_full, tables, gains, cotangent, heads, kv_heads, 1
    )
    residual_mid, cot_full = middle_scatter(
        attended, attn_full, hidden_in, cotangent, cot_near, 2
    )
    grad_mid, ffn_gain_grad, out_part, ffn_grads = feed_forward(
        residual_mid, ffn_norm, cot_full, gate_full, late_full, 3
    )

    def scatter(parts):
        return lax.psum_scatter(parts, "dp", scatter_dimension=0, tiled=True)

    ffn_sums = scatter(ffn_grads)
    total, out_near, grad_attended, attn_grads = residual_gather(
        grad_mid, residual_mid, out_part, attn_full, attended, 4
    )
    grads, attn_grads, head_gain_grads, hidden_out = attention_backward(
        normed, raw, rotated, attended, grad_attended, tables, gains,
        total, out_near, attn_grads, heads, kv_heads, 5,
    )
    attn_sums = scatter(attn_grads)
    cut = attn_norm.shape[0] // HEAD_DIM
    ready = jnp.concatenate([ffn_gain_grad.reshape(cut, HEAD_DIM), head_gain_grads])
    ready = jnp.pad(ready, ((0, -ready.shape[0] % 8), (0, 0)))
    dhidden_in, gain_sums = last_scatter(
        grads, attn_full, hidden_in, attn_norm, grad_mid, ready, 6
    )
    weights = (query_proj, key_proj, value_proj, out_proj, gate_proj, up_proj, down_proj)
    sums = deliver(ffn_sums, attn_sums, gain_sums, [weight.shape for weight in weights], cut)
    return (hidden_out, dhidden_in, *sums[:7], *(gain.reshape(-1) for gain in sums[7:]))


def solution(mesh):
    placed = (
        P(("dp", "tensor"), None),
        P("dp", "tensor"),
        P("dp", "tensor"),
        P("dp", "tensor"),
        P("tensor", "dp"),
        P("dp", "tensor"),
        P("dp", "tensor"),
        P("tensor", "dp"),
        P(),
        P(),
        P(),
        P(),
        P(("dp", "tensor"), None),
    )
    return jax.shard_map(
        per_device,
        mesh=mesh,
        in_specs=placed,
        out_specs=(
            P(("dp", "tensor"), None),
            P(("dp", "tensor"), None),
            P("dp", "tensor"),
            P("dp", "tensor"),
            P("dp", "tensor"),
            P("tensor", "dp"),
            P("dp", "tensor"),
            P("dp", "tensor"),
            P("tensor", "dp"),
            P(),
            P(),
            P(),
            P(),
        ),
        check_vma=False,
    )
```

```python
import functools
import math

import jax
import jax.numpy as jnp
from jax import lax
from jax.experimental import pallas as pl
from jax.experimental.pallas import tpu as pltpu
from jax.sharding import PartitionSpec as P


HEAD_DIM = 128
SEQ_LEN = 1024


EPSILON = 1e-06
ROPE_BASE = 1000000.0
NEG_FILL = -1e30
MESH = pl.DeviceIdType.MESH
VMEM_BYTES = 63 * 2**20
TILE = 512
F32, BF16 = jnp.float32, jnp.bfloat16
NN, NT, TN = ((1,), (0,)), ((1,), (1,)), ((0,), (0,))
IN_VMEM, IN_HBM = pl.BlockSpec(memory_space=pltpu.VMEM), pl.BlockSpec(memory_space=pl.ANY)
DMA = pltpu.SemaphoreType.DMA


def matmul(left, right, dims):
    return lax.dot_general(left, right, (dims, ((), ())), preferred_element_type=F32)


def tile_of(size):
    return TILE if size % TILE == 0 else size


def span(index, size):
    return pl.ds(pl.multiple_of(index * size, size), size)


def loop(start, stop, body):
    lax.fori_loop(start, stop, lambda index, carry: (body(index), carry)[1], 0)


def params(collective=None):
    return pltpu.CompilerParams(
        collective_id=collective, has_side_effects=True, vmem_limit_bytes=VMEM_BYTES
    )


def greet_line(here, count):
    barrier = pltpu.get_barrier_semaphore()

    @pl.when(here > 0)
    def _():
        pl.semaphore_signal(barrier, inc=1, device_id={"tensor": here - 1}, device_id_type=MESH)

    @pl.when(here < count - 1)
    def _():
        pl.semaphore_signal(barrier, inc=1, device_id={"tensor": here + 1}, device_id_type=MESH)


def meet_line(here, count):
    barrier = pltpu.get_barrier_semaphore()
    inside = jnp.logical_and(here > 0, here < count - 1)

    @pl.when(inside)
    def _():
        pl.semaphore_wait(barrier, 2)

    @pl.when(jnp.logical_not(inside))
    def _():
        pl.semaphore_wait(barrier, 1)


class LineGather:
    def __init__(self, here, count, rows, full, sems):
        self.here, self.count, self.rows, self.full, self.sems = here, count, rows, full, sems

    def copy(self, index, step, src=None):
        block = self.full.at[span(index, self.rows)]
        return pltpu.make_async_remote_copy(
            src_ref=block if src is None else src,
            dst_ref=block,
            send_sem=self.sems.at[0 if step > 0 else 1, index],
            recv_sem=self.sems.at[2, index],
            device_id={"tensor": self.here + step},
            device_id_type=MESH,
        )

    def begin(self, own=None):
        @pl.when(self.here < self.count - 1)
        def _():
            self.copy(self.here, 1, own).start()

        @pl.when(self.here > 0)
        def _():
            self.copy(self.here, -1, own).start()

    def arrive(self, hop):
        here, count = self.here, self.count

        @pl.when(here >= hop)
        def _():
            self.copy(here - hop, 1).wait_recv()

            @pl.when(here < count - 1)
            def _():
                self.copy(here - hop, 1).start()

        @pl.when(here < count - hop)
        def _():
            self.copy(here + hop, -1).wait_recv()

            @pl.when(here > 0)
            def _():
                self.copy(here + hop, -1).start()

    def each(self, hop, then):
        def side(which):
            index = self.here + (2 * which - 1) * hop
            fits = jnp.logical_and(index >= 0, index < self.count)

            @pl.when(jnp.logical_and(fits, which + hop > 0))
            def _():
                then(index)

        loop(0, 2, side)

    def pass_on(self, hop):
        here, count = self.here, self.count

        @pl.when(jnp.logical_and(here >= hop, here < count - 1))
        def _():
            self.copy(here - hop, 1).start()

        @pl.when(jnp.logical_and(here < count - hop, here > 0))
        def _():
            self.copy(here + hop, -1).start()

    def finish(self, first=0):
        here, count = self.here, self.count

        def settle(hop):
            @pl.when(jnp.logical_and(here >= hop, here < count - 1))
            def _():
                self.copy(here - hop, 1).wait_send()

            @pl.when(jnp.logical_and(here < count - hop, here > 0))
            def _():
                self.copy(here + hop, -1).wait_send()

        loop(first, count, settle)


class LineScatter:
    def __init__(self, here, count, came, going, sems):
        self.here, self.count, self.came, self.going, self.sems = here, count, came, going, sems

    def right(self, index):
        return pltpu.make_async_remote_copy(
            src_ref=self.going.at[index],
            dst_ref=self.came.at[index + 1],
            send_sem=self.sems.at[0, index],
            recv_sem=self.sems.at[1, index],
            device_id={"tensor": self.here + 1},
            device_id_type=MESH,
        )

    def left(self, index):
        return pltpu.make_async_remote_copy(
            src_ref=self.going.at[index],
            dst_ref=self.came.at[index],
            send_sem=self.sems.at[2, index],
            recv_sem=self.sems.at[3, index],
            device_id={"tensor": self.here - 1},
            device_id_type=MESH,
        )

    def goes_right(self, hop):
        return jnp.logical_and(hop >= self.here, self.here < self.count - 1)

    def goes_left(self, hop):
        return jnp.logical_and(hop >= self.count - 1 - self.here, self.here > 0)

    def rightward(self, hop):
        return self.count - 1 + self.here - hop

    def leftward(self, hop):
        return hop + self.here + 1 - self.count

    def each(self, hop, then):
        def side(which):
            goes = jnp.where(which == 0, self.goes_right(hop), self.goes_left(hop))

            @pl.when(goes)
            def _():
                then((1 - which) * self.rightward(hop) + which * self.leftward(hop))

        loop(0, 2, side)

    def add(self, index, slot):
        self.going[index] = (
            self.going[index].astype(F32) + self.came[slot].astype(F32)
        ).astype(BF16)

    def step(self, hop, send=True):
        here, count = self.here, self.count

        @pl.when(self.goes_right(hop))
        def _():
            index = self.rightward(hop)

            @pl.when(here > 0)
            def _():
                self.right(index).wait_recv()
                self.add(index, index + 1)

            if send:
                self.right(index).start()

        @pl.when(self.goes_left(hop))
        def _():
            index = self.leftward(hop)

            @pl.when(here < count - 1)
            def _():
                self.left(index).wait_recv()
                self.add(index, index)

            if send:
                self.left(index).start()

    def settle(self, hops):
        def sent(hop):
            @pl.when(self.goes_right(hop))
            def _():
                self.right(self.rightward(hop)).wait_send()

            @pl.when(self.goes_left(hop))
            def _():
                self.left(self.leftward(hop)).wait_send()

        loop(0, hops, sent)

    def finish(self, total):
        here, count = self.here, self.count

        @pl.when(here > 0)
        def _():
            self.right(here).wait_recv()
            total[...] += self.came[here + 1].astype(F32)

        @pl.when(here < count - 1)
        def _():
            self.left(here).wait_recv()
            total[...] += self.came[here].astype(F32)

        self.settle(count - 1)


class Neighbours:
    def __init__(self, here, count, to_right, to_left, lands, sems):
        self.here, self.count, self.lands, self.sems = here, count, lands, sems
        self.to_right, self.to_left = to_right, to_left

    def copy(self, side):
        return pltpu.make_async_remote_copy(
            src_ref=self.to_left if side else self.to_right,
            dst_ref=self.lands.at[side],
            send_sem=self.sems.at[0, side],
            recv_sem=self.sems.at[1, side],
            device_id={"tensor": self.here + (-1 if side else 1)},
            device_id_type=MESH,
        )

    def begin(self):
        @pl.when(self.here < self.count - 1)
        def _():
            self.copy(0).start()

        @pl.when(self.here > 0)
        def _():
            self.copy(1).start()

    def finish(self):
        @pl.when(self.here < self.count - 1)
        def _():
            self.copy(0).wait_send()
            self.copy(1).wait_recv()

        @pl.when(self.here > 0)
        def _():
            self.copy(1).wait_send()
            self.copy(0).wait_recv()


def scatter_scratch(count, rows, width):
    return [
        pltpu.VMEM((count + 1, rows, width), BF16),
        pltpu.VMEM((count, rows, width), BF16),
        DMA((4, count)),
    ]


def gather_scratch(count, rows, width):
    return [pltpu.VMEM((count * rows, width), BF16), DMA((3, count))]


def row_blocks(rows):
    return 64 if rows % 64 == 0 else rows


def norm_rows(values_ref, gain_ref, store):
    block = row_blocks(values_ref.shape[0])

    def body(index):
        rows = span(index, block)
        values = values_ref[rows, :].astype(F32)
        inverse = lax.rsqrt(jnp.mean(values * values, axis=-1, keepdims=True) + EPSILON)
        store(rows, values * inverse * gain_ref[...])

    loop(0, values_ref.shape[0] // block, body)


def norm_rows_backward(grad_ref, values_ref, gain_ref, gain_grad_ref, store):
    block = row_blocks(values_ref.shape[0])
    gain_grad_ref[...] = jnp.zeros_like(gain_grad_ref)

    def body(index):
        rows = span(index, block)
        values, grad = values_ref[rows, :].astype(F32), grad_ref[rows, :]
        inverse = lax.rsqrt(jnp.mean(values * values, axis=-1, keepdims=True) + EPSILON)
        unit = values * inverse
        grad_unit = grad * gain_ref[...]
        mean = jnp.mean(grad_unit * unit, axis=-1, keepdims=True)
        gain_grad_ref[...] += jnp.sum(grad * unit, axis=0, keepdims=True)
        store(rows, inverse * (grad_unit - unit * mean))

    loop(0, values_ref.shape[0] // block, body)


def first_kernel(
    count, hidden_ref, gain_ref, up_ref, down_ref, out_ref, late_ref, full, sems, done
):
    here = lax.axis_index("tensor")
    rows = hidden_ref.shape[0]
    greet_line(here, count)
    own = full.at[span(here, rows)]

    def store(block, normed):
        own[block, :] = normed.astype(BF16)

    norm_rows(hidden_ref, gain_ref, store)
    meet_line(here, count)
    line = LineGather(here, count, rows, full, sems)
    line.begin()
    late_ref[:, : up_ref.shape[1]] = up_ref[...]
    tile = tile_of(down_ref.shape[0])

    def turn(index):
        columns = pl.ds(pl.multiple_of(up_ref.shape[1] + index * tile, tile), tile)
        late_ref[:, columns] = jnp.transpose(down_ref[span(index, tile), :])

    loop(0, down_ref.shape[0] // tile, turn)

    def put(index):
        return pltpu.make_async_copy(
            full.at[span(index, rows)], out_ref.at[span(index, rows)], done.at[index]
        )

    def pass_on(hop):
        @pl.when(hop > 0)
        def _():
            line.arrive(hop)

        line.each(hop, lambda index: put(index).start())

    loop(0, count, pass_on)
    loop(0, count, lambda index: put(index).wait())
    line.finish()


def first_gather(hidden, gain, up, down, collective):
    count = lax.axis_size("tensor")
    rows, width = hidden.shape
    return pl.pallas_call(
        functools.partial(first_kernel, count),
        out_shape=[
            jax.ShapeDtypeStruct((count * rows, width), BF16),
            jax.ShapeDtypeStruct((up.shape[0], up.shape[1] + down.shape[0]), BF16),
        ],
        in_specs=[IN_VMEM] * 4,
        out_specs=[IN_HBM, IN_VMEM],
        scratch_shapes=gather_scratch(count, rows, width) + [DMA((count,))],
        compiler_params=params(collective),
        cost_estimate=pl.CostEstimate(
            flops=0, transcendentals=0, bytes_accessed=64 * count * rows * width
        ),
        name="first_gather",
    )(hidden, gain[None], up, down)


def middle_kernel(
    count, attended, weights, hidden_ref, cot_ref, near, mid_ref, cot_out,
    came, going, scatter_sems, full, gather_sems, done, near_done,
):
    here = lax.axis_index("tensor")
    rows, width = hidden_ref.shape
    tile = tile_of(width)
    out_columns = slice(weights.shape[1] - attended.shape[1], weights.shape[1])
    greet_line(here, count)

    def term(index, store):
        left = attended[span(index, rows), :]

        def column(k):
            store(span(k, tile), matmul(left, weights[span(k, tile), out_columns], NT))

        loop(0, width // tile, column)

    def part(index):
        def store(columns, value):
            going[index, :, columns] = value.astype(BF16)

        term(index, store)

    scatter = LineScatter(here, count, came, going, scatter_sems)
    gather = LineGather(here, count, rows, full, gather_sems)

    def put(index):
        return pltpu.make_async_copy(
            full.at[span(index, rows)], cot_out.at[span(index, rows)], done.at[index]
        )

    own = pltpu.make_async_copy(cot_ref, cot_out.at[span(here, rows)], done.at[here])
    own.start()

    def fetch(side):
        return pltpu.make_async_copy(
            near.at[side], full.at[span(here + 2 * side - 1, rows)], near_done.at[side]
        )

    def beside(then):
        @pl.when(here > 0)
        def _():
            then(0)

        @pl.when(here < count - 1)
        def _():
            then(1)

    beside(lambda side: fetch(side).start())
    scatter.each(0, part)
    meet_line(here, count)
    scatter.step(0)
    beside(lambda side: fetch(side).wait())
    gather.pass_on(1)
    gather.each(1, lambda index: put(index).start())

    def own_term(columns, value):
        mid_ref[:, columns] = hidden_ref[:, columns].astype(F32) + value

    term(here, own_term)

    def pass_on(hop):
        scatter.each(hop, part)
        scatter.step(hop)
        gather.arrive(hop + 1)
        gather.each(hop + 1, lambda index: put(index).start())

    loop(1, count - 1, pass_on)
    scatter.finish(mid_ref)
    own.wait()

    def settle(index):
        @pl.when(index != here)
        def _():
            put(index).wait()

    loop(0, count, settle)
    gather.finish(1)


def middle_scatter(attended, weights, hidden, cotangent, near, collective):
    count = lax.axis_size("tensor")
    rows, width = hidden.shape
    return pl.pallas_call(
        functools.partial(middle_kernel, count),
        out_shape=[
            jax.ShapeDtypeStruct((rows, width), F32),
            jax.ShapeDtypeStruct((count * rows, width), BF16),
        ],
        in_specs=[IN_VMEM] * 4 + [IN_HBM],
        out_specs=[IN_VMEM, IN_HBM],
        scratch_shapes=scatter_scratch(count, rows, width)
        + gather_scratch(count, rows, width)
        + [DMA((count,)), DMA((2,))],
        compiler_params=params(collective),
        cost_estimate=pl.CostEstimate(
            flops=0, transcendentals=0, bytes_accessed=80 * count * rows * width
        ),
        name="middle_scatter",
    )(attended, weights, hidden, cotangent, near)


class TileScatter:
    def __init__(self, here, count, came, going, sems):
        self.here, self.count, self.came, self.going, self.sems = here, count, came, going, sems
        self.tiles = going.shape[1]

    def right(self, index, q):
        return pltpu.make_async_remote_copy(
            src_ref=self.going.at[index, q],
            dst_ref=self.came.at[index + 1, q],
            send_sem=self.sems.at[0, index, q],
            recv_sem=self.sems.at[1, index, q],
            device_id={"tensor": self.here + 1},
            device_id_type=MESH,
        )

    def left(self, index, q):
        return pltpu.make_async_remote_copy(
            src_ref=self.going.at[index, q],
            dst_ref=self.came.at[index, q],
            send_sem=self.sems.at[2, index, q],
            recv_sem=self.sems.at[3, index, q],
            device_id={"tensor": self.here - 1},
            device_id_type=MESH,
        )

    def first(self, index, q):
        @pl.when(self.here == 0)
        def _():
            self.right(index, q).start()

        @pl.when(self.here == self.count - 1)
        def _():
            self.left(index, q).start()

    def add(self, index, q, slot):
        self.going[index, q] = (
            self.going[index, q].astype(F32) + self.came[slot, q].astype(F32)
        ).astype(BF16)

    def beats(self):
        return 2 * self.tiles + 1, self.tiles * self.count + self.count - 2

    def beat(self, time):
        here, count, tiles = self.here, self.count, self.tiles
        at = time - here
        index, q = at // tiles, at % tiles
        goes = jnp.logical_and(here > 0, jnp.logical_and(index > here, index < count))

        @pl.when(goes)
        def _():
            self.right(index, q).wait_recv()
            self.add(index, q, index + 1)
            self.right(index, q).start()

        back = time - (count - 1 - here)
        other, p = count - 1 - back // tiles, back % tiles
        comes = jnp.logical_and(here < count - 1, jnp.logical_and(other < here, other >= 0))

        @pl.when(comes)
        def _():
            self.left(other, p).wait_recv()
            self.add(other, p, other)
            self.left(other, p).start()

    def finish(self, total):
        here, count, tiles = self.here, self.count, self.tiles
        width = self.going.shape[3]

        def arrived(q):
            @pl.when(here > 0)
            def _():
                self.right(here, q).wait_recv()
                total[:, span(q, width)] += self.came[here + 1, q].astype(F32)

            @pl.when(here < count - 1)
            def _():
                self.left(here, q).wait_recv()
                total[:, span(q, width)] += self.came[here, q].astype(F32)

        loop(0, tiles, arrived)

        def settle(at):
            index, q = at // tiles, at % tiles

            @pl.when(index > here)
            def _():
                self.right(index, q).wait_send()

            @pl.when(index < here)
            def _():
                self.left(index, q).wait_send()

        loop(0, count * tiles, settle)


def ffn_kernel(
    count, mid_ref, gain_ref, cot_hbm, gate_hbm, late_hbm,
    grad_mid, gain_grad, out_part, weight_grad,
    full, gather_sems, came, going, scatter_sems,
    cot, gate_up, down_t, act, grads, stage, out_stage, loads, stores, out_store,
):
    here = lax.axis_index("tensor")
    rows, width = mid_ref.shape
    hidden = down_t.shape[1]
    cols, tile = tile_of(hidden), tile_of(width)
    at_end = jnp.logical_or(here == 0, here == count - 1)
    greet_line(here, count)
    low, high = pl.ds(0, hidden), pl.ds(hidden, hidden)
    fetches = [
        pltpu.make_async_copy(src, dst, loads.at[k])
        for k, (src, dst) in enumerate(
            (
                (cot_hbm, cot),
                (late_hbm.at[:, high], down_t),
                (gate_hbm, gate_up.at[:, low]),
                (late_hbm.at[:, low], gate_up.at[:, high]),
            )
        )
    ]
    for fetch in fetches:
        fetch.start()
    own = full.at[span(here, rows)]

    def store_normed(block, normed):
        own[block, :] = normed.astype(BF16)

    norm_rows(mid_ref, gain_ref, store_normed)
    meet_line(here, count)
    gather = LineGather(here, count, rows, full, gather_sems)
    scatter = TileScatter(here, count, came, going, scatter_sems)
    gather.begin()
    fetches[0].wait()
    fetches[1].wait()

    def grad_hidden(index):
        block, columns = span(index // (hidden // cols), rows), span(index % (hidden // cols), cols)
        grads[block, columns] = matmul(cot[block, :], down_t[:, columns], NN).astype(BF16)

    loop(0, count * (hidden // cols), grad_hidden)
    fetches[2].wait()
    fetches[3].wait()

    def out_copy(index):
        return pltpu.make_async_copy(out_stage, out_part.at[span(index, rows)], out_store.at[0])

    def output(index):
        block = span(index, rows)

        def column(k):
            out_stage[:, span(k, tile)] = matmul(
                act[block, :], down_t[span(k, tile), :], NT
            ).astype(BF16)

        loop(0, width // tile, column)
        out_copy(index).start()
        out_copy(index).wait()

    def work(index):
        block = span(index, rows)

        def column(k):
            here_cols, up_cols = span(k, cols), pl.ds(pl.multiple_of(hidden + k * cols, cols), cols)
            gate = matmul(full[block, :], gate_up[:, here_cols], NN)
            up = matmul(full[block, :], gate_up[:, up_cols], NN)
            grad = grads[block, here_cols].astype(F32)
            sigmoid = jax.nn.sigmoid(gate)
            silu = gate * sigmoid
            act[block, here_cols] = (silu * up).astype(BF16)
            grads[block, up_cols] = (grad * silu).astype(BF16)
            grads[block, here_cols] = (
                grad * up * sigmoid * (1.0 + gate * (1.0 - sigmoid))
            ).astype(BF16)

        loop(0, hidden // cols, column)

        def term(q):
            value = matmul(grads[block, :], gate_up[span(q, tile), :], NT)

            @pl.when(index == here)
            def _():
                grad_mid[:, span(q, tile)] = value

            @pl.when(index != here)
            def _():
                going[index, q] = value.astype(BF16)
                scatter.first(index, q)

        loop(0, width // tile, term)

        @pl.when(at_end)
        def _():
            output(index)

    def pass_on(hop):
        @pl.when(hop > 0)
        def _():
            gather.arrive(hop)

        gather.each(hop, work)

    loop(0, count, pass_on)
    across, wide = width // tile, hidden // cols
    down_jobs = across * wide

    def put(slot, target):
        return pltpu.make_async_copy(stage.at[slot], target, stores.at[slot])

    def job(index):
        slot = index % 2

        @pl.when(index >= 2)
        def _():
            put(slot, weight_grad.at[span(0, tile), span(0, cols)]).wait()

        @pl.when(index < down_jobs)
        def _():
            i, k = index // wide, index % wide
            stage[slot] = matmul(cot[:, span(i, tile)], act[:, span(k, cols)], TN).astype(BF16)
            put(slot, weight_grad.at[span(i, tile), span(2 * wide + k, cols)]).start()

        @pl.when(index >= down_jobs)
        def _():
            i, k = (index - down_jobs) // (2 * wide), (index - down_jobs) % (2 * wide)
            stage[slot] = matmul(full[:, span(i, tile)], grads[:, span(k, cols)], TN).astype(BF16)
            put(slot, weight_grad.at[span(i, tile), span(k, cols)]).start()

    jobs = 3 * down_jobs
    start, stop = scatter.beats()
    each = -(-jobs // max(1, stop - start))

    def beat(time):
        scatter.beat(time)

        @pl.when(jnp.logical_and(time - start < count, jnp.logical_not(at_end)))
        def _():
            output(time - start)

        loop((time - start) * each, jnp.minimum((time - start + 1) * each, jobs), job)

    loop(start, stop, beat)
    for slot in range(2):
        put(slot, weight_grad.at[span(0, tile), span(0, cols)]).wait()
    scatter.finish(grad_mid)
    gather.finish()

    def store_grad(block, value):
        rows_here = pl.ds(here * rows + block.start, block.size)
        grad_mid[block, :] = cot[rows_here, :].astype(F32) + value

    norm_rows_backward(grad_mid, mid_ref, gain_ref, gain_grad, store_grad)


def feed_forward(mid, gain, cot_full, gate, late, collective):
    count = lax.axis_size("tensor")
    rows, width = mid.shape
    hidden = gate.shape[1]
    everything, tile = count * rows, tile_of(width)
    tiles = width // tile
    return pl.pallas_call(
        functools.partial(ffn_kernel, count),
        out_shape=[
            jax.ShapeDtypeStruct((rows, width), F32),
            jax.ShapeDtypeStruct((1, width), F32),
            jax.ShapeDtypeStruct((everything, width), BF16),
            jax.ShapeDtypeStruct((width, 3 * hidden), BF16),
        ],
        in_specs=[IN_VMEM, IN_VMEM, IN_HBM, IN_HBM, IN_HBM],
        out_specs=[IN_VMEM, IN_VMEM, IN_HBM, IN_HBM],
        scratch_shapes=gather_scratch(count, rows, width)
        + [
            pltpu.VMEM((count + 1, tiles, rows, tile), BF16),
            pltpu.VMEM((count, tiles, rows, tile), BF16),
            DMA((4, count, tiles)),
            pltpu.VMEM((everything, width), BF16),
            pltpu.VMEM((width, 2 * hidden), BF16),
            pltpu.VMEM((width, hidden), BF16),
            pltpu.VMEM((everything, hidden), BF16),
            pltpu.VMEM((everything, 2 * hidden), BF16),
            pltpu.VMEM((2, tile, tile_of(hidden)), BF16),
            pltpu.VMEM((rows, width), BF16),
            DMA((4,)),
            DMA((2,)),
            DMA((1,)),
        ],
        compiler_params=params(collective),
        cost_estimate=pl.CostEstimate(
            flops=18 * everything * width * hidden,
            transcendentals=everything * hidden,
            bytes_accessed=160 * everything * width,
        ),
        name="feed_forward",
    )(mid, gain[None], cot_full, gate, late)


def last_kernel(
    count, planes, grads, weights, hidden_ref, gain_ref, grad_mid, ready_ref, hidden_grad, sums_ref,
    came, going, scatter_sems, total, gain_grad, gains, line_sum, line_slots, slots, line_sems, sems,
):
    here = lax.axis_index("tensor")
    plane = lax.axis_index("dp")
    barrier = pltpu.get_barrier_semaphore()

    def others(total, me, then):
        def body(index):
            @pl.when(index != me)
            def _():
                then(index)

        loop(0, total, body)

    def greet(axis):
        def signal(index):
            pl.semaphore_signal(barrier, inc=1, device_id={axis: index}, device_id_type=MESH)

        return signal

    others(count, here, greet("tensor"))
    others(planes, plane, greet("dp"))

    def add_up(axis, total, me, source, slots, sems):
        def give(index, slot):
            return pltpu.make_async_remote_copy(
                src_ref=source,
                dst_ref=slots.at[slot],
                send_sem=sems.at[0, index],
                recv_sem=sems.at[1, slot],
                device_id={axis: index},
                device_id_type=MESH,
            )

        others(total, me, lambda index: give(index, me).start())
        slots[me] = source[...]

        def settle(index):
            give(index, index).wait_recv()
            give(index, me).wait_send()

        others(total, me, settle)
        return lax.fori_loop(1, total, lambda index, so_far: so_far + slots[index], slots[0])

    rows, width = hidden_ref.shape
    tile = tile_of(width)

    def term(index, store):
        left = grads[span(index, rows), :]

        def column(k):
            store(span(k, tile), matmul(left, weights[span(k, tile), : left.shape[1]], NT))

        loop(0, width // tile, column)

    def part(index):
        def store(columns, value):
            going[index, :, columns] = value.astype(BF16)

        term(index, store)

    def own_term(columns, value):
        total[:, columns] = value

    scatter = LineScatter(here, count, came, going, scatter_sems)
    scatter.each(0, part)
    pl.semaphore_wait(barrier, count + planes - 2)
    scatter.step(0)
    late = width // HEAD_DIM
    gains[late:, :] = ready_ref[...]
    term(here, own_term)

    def scatter_hop(hop):
        scatter.each(hop, part)
        scatter.step(hop)

    loop(1, count - 1, scatter_hop)
    scatter.finish(total)

    def store_grad(block, value):
        hidden_grad[block, :] = (grad_mid[block, :] + value).astype(BF16)

    norm_rows_backward(total, hidden_ref, gain_ref, gain_grad, store_grad)
    for k in range(late):
        gains[k : k + 1, :] = gain_grad[:, k * HEAD_DIM : (k + 1) * HEAD_DIM]
    line_sum[...] = add_up("tensor", count, here, gains, line_slots, line_sems)
    sums_ref[...] = add_up("dp", planes, plane, line_sum, slots, sems)


def last_scatter(grads, weights, hidden, gain, grad_mid, ready, collective):
    count, planes = lax.axis_size("tensor"), lax.axis_size("dp")
    gains = (gain.shape[0] // HEAD_DIM + ready.shape[0], HEAD_DIM)
    rows, width = hidden.shape
    return pl.pallas_call(
        functools.partial(last_kernel, count, planes),
        out_shape=[
            jax.ShapeDtypeStruct((rows, width), BF16),
            jax.ShapeDtypeStruct(gains, F32),
        ],
        in_specs=[IN_VMEM] * 6,
        out_specs=[IN_VMEM] * 2,
        scratch_shapes=scatter_scratch(count, rows, width)
        + [
            pltpu.VMEM((rows, width), F32),
            pltpu.VMEM((1, width), F32),
            pltpu.VMEM(gains, F32),
            pltpu.VMEM(gains, F32),
            pltpu.VMEM((count,) + gains, F32),
            pltpu.VMEM((planes,) + gains, F32),
            DMA((2, count)),
            DMA((2, planes)),
        ],
        compiler_params=params(collective),
        cost_estimate=pl.CostEstimate(
            flops=0, transcendentals=0, bytes_accessed=64 * count * rows * width
        ),
        name="last_scatter",
    )(grads, weights, hidden, gain[None], grad_mid, ready)


def rope_of(values, cosine, signed_sine):
    return values * cosine + pltpu.roll(values, HEAD_DIM // 2, 1) * signed_sine


def rope_back(grad, cosine, signed_sine):
    return grad * cosine - pltpu.roll(grad, HEAD_DIM // 2, 1) * signed_sine


def head_columns(index):
    return pl.ds(pl.multiple_of(index * HEAD_DIM, HEAD_DIM), HEAD_DIM)


def attention_kernel(
    count, heads, kv_heads, sequence, normed_hbm, weights_hbm, cosine, signed_sine, query_gain, key_gain, cot_hbm,
    raw, rotated, attended, near, normed, weights, loads, sems,
):
    here_on_line = lax.axis_index("tensor")
    greet_line(here_on_line, count)
    rows = normed.shape[0]
    width = (heads + 2 * kv_heads) * HEAD_DIM
    block = math.gcd(rows, 256)
    get_weights = pltpu.make_async_copy(weights_hbm.at[:, pl.ds(0, width)], weights, loads.at[0])
    get_normed = pltpu.make_async_copy(normed_hbm, normed, loads.at[1])
    get_weights.start()
    get_normed.start()
    meet_line(here_on_line, count)
    hop = Neighbours(here_on_line, count, cot_hbm, cot_hbm, near, sems)
    hop.begin()
    get_weights.wait()
    get_normed.wait()
    positions = sequence // block

    def project(index):
        here = span(index, block)
        table = span(index % positions, block)
        cos, sin = cosine[table, :], signed_sine[table, :]
        left = normed[here, :]
        groups = 4 if (heads + kv_heads) % 4 == 0 and (2 * kv_heads) % 4 == 0 else 1
        for first in range(0, heads + 2 * kv_heads, groups):
            several = slice(first * HEAD_DIM, (first + groups) * HEAD_DIM)
            made = matmul(left, weights[:, several], NN)
            for k in range(groups):
                head = first + k
                columns = slice(head * HEAD_DIM, (head + 1) * HEAD_DIM)
                value = made[:, k * HEAD_DIM : (k + 1) * HEAD_DIM]
                if head < heads + kv_heads:
                    raw[here, columns] = value
                    gain = query_gain if head < heads else key_gain
                    inverse = lax.rsqrt(
                        jnp.mean(value * value, axis=-1, keepdims=True) + EPSILON
                    )
                    value = rope_of(value * inverse * gain[...], cos, sin)
                rotated[here, columns] = value.astype(BF16)

    loop(0, rows // block, project)
    scale = 1.0 / math.sqrt(HEAD_DIM)

    def one_head(index):
        start, head = (index // heads) * sequence, index % heads
        kv = head // (heads // kv_heads)
        for k in range(positions):
            length = (k + 1) * block
            here = pl.ds(pl.multiple_of(start + k * block, block), block)
            keys = pl.ds(pl.multiple_of(start, block), length)
            query = rotated[here, head_columns(head)]
            scores = matmul(query, rotated[keys, head_columns(heads + kv)], NT) * scale
            at_row = lax.broadcasted_iota(jnp.int32, scores.shape, 0) + k * block
            at_column = lax.broadcasted_iota(jnp.int32, scores.shape, 1)
            scores = jnp.where(at_column <= at_row, scores, NEG_FILL)
            powers = jnp.exp(scores - jnp.max(scores, axis=-1, keepdims=True))
            probs = powers * (1.0 / jnp.sum(powers, axis=-1, keepdims=True))
            attended[here, head_columns(head)] = matmul(
                probs.astype(BF16), rotated[keys, head_columns(heads + kv_heads + kv)], NN
            ).astype(BF16)

    loop(0, (rows // sequence) * heads, one_head)
    hop.finish()


def attention_forward(normed, weights, tables, gains, cotangent, heads, kv_heads, collective):
    count = lax.axis_size("tensor")
    rows, width = normed.shape
    across = (heads + 2 * kv_heads) * HEAD_DIM
    return pl.pallas_call(
        functools.partial(attention_kernel, count, heads, kv_heads, SEQ_LEN),
        out_shape=[
            jax.ShapeDtypeStruct((rows, (heads + kv_heads) * HEAD_DIM), F32),
            jax.ShapeDtypeStruct((rows, across), BF16),
            jax.ShapeDtypeStruct((rows, heads * HEAD_DIM), BF16),
            jax.ShapeDtypeStruct((2,) + cotangent.shape, BF16),
        ],
        in_specs=[IN_HBM] * 2 + [IN_VMEM] * 4 + [IN_HBM],
        out_specs=[IN_VMEM] * 3 + [IN_HBM],
        scratch_shapes=[
            pltpu.VMEM((rows, width), BF16),
            pltpu.VMEM((width, across), BF16),
            DMA((2,)),
            DMA((2, 2)),
        ],
        compiler_params=params(collective),
        cost_estimate=pl.CostEstimate(
            flops=2 * rows * width * across,
            transcendentals=rows * SEQ_LEN * heads,
            bytes_accessed=20 * rows * width,
        ),
        name="attention_forward",
    )(normed, weights, *tables, *gains, cotangent)


def attention_back_kernel(
    count, heads, kv_heads, sequence, grad_ref, mid_ref, part_hbm, weights_hbm, normed_hbm,
    raw, rotated, attended, cosine, signed_sine, query_gain, key_gain,
    grads, weight_grad, gain_grad, hidden_out,
    full, gather_sems, came, going, scatter_sems,
    total, out_t, normed, grad_rot, grad_heads, stage, loads, part_loads, stores,
):
    here = lax.axis_index("tensor")
    rows, width = mid_ref.shape
    positions = sequence // rows
    greet_line(here, count)
    out_width = attended.shape[1]
    out_columns = pl.ds(weights_hbm.shape[1] - out_width, out_width)
    get_out = pltpu.make_async_copy(weights_hbm.at[:, out_columns], out_t, loads.at[0])
    get_normed = pltpu.make_async_copy(normed_hbm, normed, loads.at[1])
    get_out.start()

    def fetch(index):
        return pltpu.make_async_copy(
            part_hbm.at[span(index, rows)], going.at[index], part_loads.at[index]
        )

    loop(0, count, lambda index: fetch(index).start())
    get_normed.start()
    full[span(here, rows), :] = grad_ref[...].astype(BF16)
    gather = LineGather(here, count, rows, full, gather_sems)
    scatter = LineScatter(here, count, came, going, scatter_sems)
    meet_line(here, count)
    gather.begin()
    loop(0, count, lambda index: fetch(index).wait())
    scatter.step(0)
    total[...] = mid_ref[...] + going[here].astype(F32)
    scale = 1.0 / math.sqrt(HEAD_DIM)
    grad_rot[:, heads * HEAD_DIM :] = jnp.zeros_like(grad_rot[:, heads * HEAD_DIM :])
    get_out.wait()

    def one_head(block, start, k, head):
        kv = head // (heads // kv_heads)
        key_columns, value_columns = head_columns(heads + kv), head_columns(heads + kv_heads + kv)
        length = (k + 1) * rows
        keys = pl.ds(pl.multiple_of(start, rows), length)
        query, key = rotated[block, head_columns(head)], rotated[keys, key_columns]
        grad = grad_heads[:, head_columns(head)]
        scores = matmul(key, query, NT) * scale
        at_key = lax.broadcasted_iota(jnp.int32, scores.shape, 0)
        at_query = lax.broadcasted_iota(jnp.int32, scores.shape, 1) + k * rows
        scores = jnp.where(at_key <= at_query, scores, NEG_FILL)
        powers = jnp.exp(scores - jnp.max(scores, axis=0, keepdims=True))
        probs = powers * (1.0 / jnp.sum(powers, axis=0, keepdims=True))
        product = grad.astype(F32) * attended[block, head_columns(head)].astype(F32)
        delta = jnp.sum(jnp.transpose(product), axis=0, keepdims=True)
        grad_rot[keys, value_columns] += matmul(probs.astype(BF16), grad, NN)
        grad_probs = matmul(rotated[keys, value_columns], grad, NT)
        grad_scores = (probs * (grad_probs - delta) * scale).astype(BF16)
        grad_rot[keys, key_columns] += matmul(grad_scores, query, NN)
        grad_rot[block, head_columns(head)] = matmul(grad_scores, key, TN)

    def work(index):
        block, start = span(index, rows), (index // positions) * sequence
        grad_heads[...] = matmul(full[block, :], out_t[...], NN).astype(BF16)
        for k in range(positions):

            @pl.when(index % positions == k)
            def _():
                loop(0, heads, lambda head: one_head(block, start, k, head))

    def pass_on(hop):
        @pl.when(hop > 0)
        def _():
            gather.arrive(hop)

        gather.each(hop, work)

        @pl.when(jnp.logical_and(hop > 0, hop < count - 1))
        def _():
            scatter.step(hop)

    loop(0, count, pass_on)
    gain_grad[...] = jnp.zeros_like(gain_grad)

    def unrotate(index):
        block, table = span(index, rows), span(index % positions, rows)
        cos, sin = cosine[table, :], signed_sine[table, :]
        for head in range(heads + 2 * kv_heads):
            columns = slice(head * HEAD_DIM, (head + 1) * HEAD_DIM)
            grad = grad_rot[block, columns]
            if head < heads + kv_heads:
                which = 0 if head < heads else 1
                gain = query_gain if head < heads else key_gain
                grad = rope_back(grad, cos, sin)
                value = raw[block, columns]
                inverse = lax.rsqrt(jnp.mean(value * value, axis=-1, keepdims=True) + EPSILON)
                unit = value * inverse
                gain_grad[which : which + 1, :] += jnp.sum(grad * unit, axis=0, keepdims=True)
                grad_unit = grad * gain[...]
                mean = jnp.mean(grad_unit * unit, axis=-1, keepdims=True)
                grad = inverse * (grad_unit - unit * mean)
            grads[block, columns] = grad.astype(BF16)

    loop(0, count, unrotate)
    get_normed.wait()
    tile, cols = stage.shape[1:]
    wide = grads.shape[1] // cols

    def target(index):
        return weight_grad.at[span(index // wide, tile), span(index % wide, cols)]

    def put(index):
        return pltpu.make_async_copy(stage.at[index % 2], target(index), stores.at[index % 2])

    tiles = width // tile * wide

    def weight_tile(index):
        @pl.when(index >= 2)
        def _():
            put(index - 2).wait()

        left, right = normed[:, span(index // wide, tile)], grads[:, span(index % wide, cols)]
        stage[index % 2] = matmul(left, right, TN).astype(BF16)
        put(index).start()

    loop(0, tiles, weight_tile)

    def column(k):
        out_t[span(k, tile), :] = matmul(full[:, span(k, tile)], attended[...], TN).astype(BF16)

    loop(0, width // tile, column)
    put_out = pltpu.make_async_copy(out_t, weight_grad.at[:, out_columns], loads.at[0])
    put_out.start()
    for index in range(max(0, tiles - 2), tiles):
        put(index).wait()
    scatter.finish(total)
    gather.finish()
    hidden_out[...] = total[...].astype(BF16)
    put_out.wait()


def attention_backward(grad_mid, mid, out_part, weights, normed, raw, rotated, attended, tables, gains, heads, kv_heads, collective):
    count = lax.axis_size("tensor")
    rows, width = mid.shape
    everything, across = count * rows, (heads + 2 * kv_heads) * HEAD_DIM
    return pl.pallas_call(
        functools.partial(attention_back_kernel, count, heads, kv_heads, SEQ_LEN),
        out_shape=[
            jax.ShapeDtypeStruct((everything, across), BF16),
            jax.ShapeDtypeStruct(weights.shape, BF16),
            jax.ShapeDtypeStruct((2, HEAD_DIM), F32),
            jax.ShapeDtypeStruct((rows, width), BF16),
        ],
        in_specs=[IN_VMEM] * 2 + [IN_HBM] * 3 + [IN_VMEM] * 7,
        out_specs=[IN_VMEM, IN_HBM, IN_VMEM, IN_VMEM],
        scratch_shapes=gather_scratch(count, rows, width)
        + scatter_scratch(count, rows, width)
        + [
            pltpu.VMEM((rows, width), F32),
            pltpu.VMEM((width, attended.shape[1]), BF16),
            pltpu.VMEM((everything, width), BF16),
            pltpu.VMEM((everything, across), F32),
            pltpu.VMEM((rows, attended.shape[1]), BF16),
            pltpu.VMEM((2, tile_of(width), tile_of(across)), BF16),
            DMA((2,)),
            DMA((count,)),
            DMA((2,)),
        ],
        compiler_params=params(collective),
        cost_estimate=pl.CostEstimate(
            flops=4 * everything * width * across,
            transcendentals=everything * SEQ_LEN * heads,
            bytes_accessed=80 * everything * width,
        ),
        name="attention_backward",
    )(grad_mid, mid, out_part, weights, normed, raw, rotated, attended, *tables, *gains)


def deliver_kernel(ffn_sums, attn_sums, gains, *outs):
    query, key, value, out, gate, up, down, attn_gain, query_gain, key_gain, ffn_gain = outs

    def turned(source, first, target):
        side = tile_of(target.shape[0])
        for k in range(target.shape[0] // side):
            columns = slice(first + k * side, first + (k + 1) * side)
            target[k * side : (k + 1) * side, :] = jnp.transpose(source[:, columns].astype(F32))

    start = 0
    for target in (query, key, value):
        target[...] = attn_sums[:, start : start + target.shape[1]].astype(F32)
        start += target.shape[1]
    turned(attn_sums, start, out)
    width = gate.shape[1]
    gate[...] = ffn_sums[:, :width].astype(F32)
    up[...] = ffn_sums[:, width : 2 * width].astype(F32)
    turned(ffn_sums, 2 * width, down)
    cut = attn_gain.shape[0]
    attn_gain[...] = gains[:cut, :]
    ffn_gain[...] = gains[cut : 2 * cut, :]
    query_gain[...] = gains[2 * cut : 2 * cut + 1, :]
    key_gain[...] = gains[2 * cut + 1 : 2 * cut + 2, :]


def deliver(ffn_sums, attn_sums, gains, shapes, cut):
    shapes = list(shapes) + [(cut, HEAD_DIM), (1, HEAD_DIM), (1, HEAD_DIM), (cut, HEAD_DIM)]
    return pl.pallas_call(
        deliver_kernel,
        out_shape=[jax.ShapeDtypeStruct(shape, F32) for shape in shapes],
        in_specs=[IN_VMEM] * 3,
        out_specs=[IN_VMEM] * len(shapes),
        compiler_params=pltpu.CompilerParams(vmem_limit_bytes=VMEM_BYTES),
        name="deliver",
    )(ffn_sums, attn_sums, gains)


def rope_tables(positions, width):
    half_width = width // 2
    freqs = ROPE_BASE ** (-(jnp.arange(half_width, dtype=F32) * (2.0 / width)))
    angles = positions.astype(F32)[:, None] * freqs[None, :]
    cosine, sine = jnp.cos(angles), jnp.sin(angles)
    return (
        jnp.concatenate([cosine, cosine], axis=1),
        jnp.concatenate([-sine, sine], axis=1),
    )


def per_device(
    hidden_in,
    query_proj,
    key_proj,
    value_proj,
    out_proj,
    gate_proj,
    up_proj,
    down_proj,
    attn_norm,
    query_norm,
    key_norm,
    ffn_norm,
    cotangent,
):
    heads_width, kv_width = query_proj.shape[1], key_proj.shape[1]
    heads, kv_heads = heads_width // HEAD_DIM, kv_width // HEAD_DIM
    attn_full = lax.all_gather(
        jnp.concatenate([query_proj, key_proj, value_proj, out_proj.T], axis=1),
        "dp",
        axis=0,
        tiled=True,
    )
    gate_full = lax.all_gather(gate_proj, "dp", axis=0, tiled=True)
    normed, late = first_gather(hidden_in, attn_norm, up_proj, down_proj, 0)
    late_full = lax.all_gather(late, "dp", axis=0, tiled=True)
    tables = rope_tables(jnp.arange(SEQ_LEN), HEAD_DIM)
    gains = (query_norm[None], key_norm[None])
    raw, rotated, attended, cot_near = attention_forward(
        normed, attn_full, tables, gains, cotangent, heads, kv_heads, 1
    )
    residual_mid, cot_full = middle_scatter(
        attended, attn_full, hidden_in, cotangent, cot_near, 2
    )
    grad_mid, ffn_gain_grad, out_part, ffn_grads = feed_forward(
        residual_mid, ffn_norm, cot_full, gate_full, late_full, 3
    )

    def scatter(parts):
        return lax.psum_scatter(parts, "dp", scatter_dimension=0, tiled=True)

    ffn_sums = scatter(ffn_grads)
    grads, attn_grads, head_gain_grads, hidden_out = attention_backward(
        grad_mid, residual_mid, out_part, attn_full, normed, raw, rotated, attended,
        tables, gains, heads, kv_heads, 4,
    )
    attn_sums = scatter(attn_grads)
    cut = attn_norm.shape[0] // HEAD_DIM
    ready = jnp.concatenate([ffn_gain_grad.reshape(cut, HEAD_DIM), head_gain_grads])
    ready = jnp.pad(ready, ((0, -ready.shape[0] % 8), (0, 0)))
    dhidden_in, gain_sums = last_scatter(
        grads, attn_full, hidden_in, attn_norm, grad_mid, ready, 5
    )
    weights = (query_proj, key_proj, value_proj, out_proj, gate_proj, up_proj, down_proj)
    sums = deliver(ffn_sums, attn_sums, gain_sums, [weight.shape for weight in weights], cut)
    return (hidden_out, dhidden_in, *sums[:7], *(gain.reshape(-1) for gain in sums[7:]))


def solution(mesh):
    placed = (
        P(("dp", "tensor"), None),
        P("dp", "tensor"),
        P("dp", "tensor"),
        P("dp", "tensor"),
        P("tensor", "dp"),
        P("dp", "tensor"),
        P("dp", "tensor"),
        P("tensor", "dp"),
        P(),
        P(),
        P(),
        P(),
        P(("dp", "tensor"), None),
    )
    return jax.shard_map(
        per_device,
        mesh=mesh,
        in_specs=placed,
        out_specs=(
            P(("dp", "tensor"), None),
            P(("dp", "tensor"), None),
            P("dp", "tensor"),
            P("dp", "tensor"),
            P("dp", "tensor"),
            P("tensor", "dp"),
            P("dp", "tensor"),
            P("dp", "tensor"),
            P("tensor", "dp"),
            P(),
            P(),
            P(),
            P(),
        ),
        check_vma=False,
    )
```
